32 devices in a mesh: sub: 4 (over z), ma: 8 (over y, x, core).
Axes of the slice: x: 2, y: 2, z: 4, core: 2. Of those that a mesh axis runs over, the one named last changes fastest.
Arguments:
- forcing: float32 [2, 256, 2, 64, 512], P(None, 'sub', None, 'ma'), may hold values from -24 to 24
- slot_wavenumber: int32 [64], P('ma'), may hold values from 0 to 511, as said below
- inverse: float32 [4, 2, 64, 64, 512], P('sub'), may hold values from -2 to 2
- edge_weights: float32 [4, 2, 64], P('sub'), may hold values from -1357 to 1357, as said below
Outputs:
- transform_field: float32 [2, 256, 2, 64, 512], P(None, ('sub', 'ma'))
The draws below stay inside these ranges and needn't reach their ends.
Inputs may be any that keep to these rules, and one draw needn't show every extreme that they name: `slot_wavenumber`: each device's slots hold 4 pairs: slots 2j and 2j + 1 carry a wavenumber m below 256 and 511 - m, in that order; no wavenumber appears twice. `edge_weights`: together with inverse it makes every row of the interface system strictly diagonally dominant with a positive diagonal.
All inputs are finite; a program needn't handle non-finite values.
Results may differ from the reference program's by a relative error of at most 0.0003.
Values sent between devices are 32-bit elements; how exact they have to be, the bound alone decides.
A program may use at most 192 MiB of HBM per device.

```python
import math
import jax
import jax.numpy as jnp
from jax import lax

P_SIZE = 64
L = 512
FIELDS = 2
NSUB = 4
MTOT = 64
NR = 256


def shell_radius(key):
    widths = jax.random.uniform(jax.random.fold_in(key, 11), (NSUB,), jnp.float32, 1.0, 2.0)
    widths = 0.65 * widths / jnp.sum(widths)
    starts = 0.35 + jnp.cumsum(widths) - widths
    spacing = jnp.arange(P_SIZE, dtype=jnp.float32) / (P_SIZE - 1)
    return (starts[:, None] + widths[:, None] * spacing[None, :], widths)


def draw_slot_wavenumber(key, part):
    halfway = L // 2
    chosen = jax.random.permutation(jax.random.fold_in(key, 21), halfway)[:MTOT // 2]
    paired = jnp.stack([chosen, L - 1 - chosen], axis=1).reshape(MTOT)
    return paired.astype(jnp.int32)


def draw_edge_weights(key, part):
    radius, widths = shell_radius(key)
    step_size = widths / (P_SIZE - 1)
    lower_row = jnp.zeros((NSUB, P_SIZE), jnp.float32)
    lower_row = lower_row.at[:, 0].set(-1.5 / step_size).at[:, 1].set(2.0 / step_size).at[:, 2].set(-0.5 / step_size)
    upper_row = jnp.zeros((NSUB, P_SIZE), jnp.float32)
    upper_row = upper_row.at[:, P_SIZE - 1].set(1.5 / step_size).at[:, P_SIZE - 2].set(-2.0 / step_size).at[:, P_SIZE - 3].set(0.5 / step_size)
    return jnp.stack([lower_row, upper_row], axis=1)


def draw_inverse(key, part):
    radius, widths = shell_radius(key)
    field_scale = jnp.exp(jax.random.uniform(jax.random.fold_in(key, 12), (FIELDS,), jnp.float32, math.log(0.05), math.log(0.5)))
    degree_scale = jnp.exp(jax.random.uniform(jax.random.fold_in(key, 13), (FIELDS, L), jnp.float32, 0.0, math.log(3.0)))
    strength = (field_scale[:, None] * degree_scale)[None, :, :, None]
    degree = jnp.arange(L, dtype=jnp.float32)
    angular = degree * (degree + 1.0)
    inner = radius[:, 1:-1]
    below_gap = radius[:, 1:-1] - radius[:, :-2]
    above_gap = radius[:, 2:] - radius[:, 1:-1]
    spans = below_gap + above_gap
    sub_coef = 2.0 / (below_gap * spans) - 2.0 / (inner * spans)
    sup_coef = 2.0 / (above_gap * spans) + 2.0 / (inner * spans)
    mid_coef = 2.0 / (below_gap * above_gap)
    lower_band = -strength * sub_coef[:, None, None, :]
    upper_band = -strength * sup_coef[:, None, None, :]
    main_band = 1.0 + strength * (mid_coef[:, None, None, :] + angular[None, None, :, None] / (inner[:, None, None, :] * inner[:, None, None, :]))
    edges = ((0, 0), (0, 0), (0, 0), (1, 1))
    lower_band = jnp.pad(lower_band, edges)
    upper_band = jnp.pad(upper_band, edges)
    main_band = jnp.pad(main_band, edges, constant_values=1.0)
    bands = (jnp.moveaxis(lower_band, -1, 0), jnp.moveaxis(main_band, -1, 0), jnp.moveaxis(upper_band, -1, 0), jnp.eye(P_SIZE, dtype=jnp.float32))

    def forward(state_pair, inputs):
        prior_ratio, prior_value = state_pair
        sub_entry, main_entry, sup_entry, unit_row = inputs
        pivot_value = main_entry - sub_entry * prior_ratio
        ratio_next = sup_entry / pivot_value
        value_next = (unit_row[None, None, None, :] - sub_entry[..., None] * prior_value) / pivot_value[..., None]
        return ((ratio_next, value_next), (ratio_next, value_next))
    initial = (jnp.zeros((NSUB, FIELDS, L), jnp.float32), jnp.zeros((NSUB, FIELDS, L, P_SIZE), jnp.float32))
    _, (ratios, values) = lax.scan(forward, initial, bands)

    def backward(later_value, inputs):
        ratio_here, value_here = inputs
        current = value_here - ratio_here[..., None] * later_value
        return (current, current)
    _, solved = lax.scan(backward, jnp.zeros((NSUB, FIELDS, L, P_SIZE), jnp.float32), (ratios, values), reverse=True)
    position = jnp.arange(P_SIZE)
    interior = ((position > 0) & (position < P_SIZE - 1)).astype(jnp.float32)
    noise = jax.random.truncated_normal(jax.random.fold_in(key, 14), -3.0, 3.0, (NSUB, FIELDS, P_SIZE, P_SIZE, L), jnp.float32)
    inner_mask = (interior[:, None] * interior[None, :])[None, None, :, :, None]
    mixing = jnp.eye(P_SIZE, dtype=jnp.float32)[None, None, :, :, None] + 0.5 * noise / math.sqrt(P_SIZE - 2) * inner_mask
    return jnp.einsum('isflk,sfkjl->sfijl', solved, mixing, precision=lax.Precision.HIGHEST)


def block_levels(rng, dims, split, smallest, largest):
    def one(dim, blocks):
        draws = jax.random.uniform(jax.random.fold_in(jax.random.fold_in(rng, 6), dim), (blocks,), jnp.float32, smallest / len(split), largest / len(split))
        return jnp.repeat(jnp.exp(draws), dims[dim] // blocks).reshape((-1,) + (1,) * (len(dims) - dim - 1))

    loudness = one(*split[0])
    for cut in split[1:]:
        loudness = loudness * one(*cut)
    return loudness


def scatter_about(key, shape, scale, most, split=(), held_as=jnp.bfloat16):
    drawn = scale * jax.random.normal(key, shape, jnp.float32)
    if split:
        drawn = drawn * block_levels(key, shape, split, -0.22, 0.18)
    return jnp.clip(drawn, -most, most).astype(held_as)


def setup_inputs(seed: int = 0) -> dict:
    arg_keys = jax.random.split(jax.random.key(seed), 5)
    forcing = scatter_about(arg_keys[0], (FIELDS, NR, 2, MTOT, L), 4.0, 24.0, ((1, 4), (3, 8)), jnp.float32)
    slot_wavenumber = draw_slot_wavenumber(jax.random.fold_in(arg_keys[4], 71), 0)
    inverse = draw_inverse(jax.random.fold_in(arg_keys[4], 71), 0)
    edge_weights = draw_edge_weights(jax.random.fold_in(arg_keys[4], 71), 0)
    return {"forcing": forcing, "slot_wavenumber": slot_wavenumber, "inverse": inverse, "edge_weights": edge_weights}


HIGH = lax.Precision.HIGHEST


def local_solve(pair):
    block_inverse, block_source = pair
    return jnp.einsum('fpql,fqcml->fpcml', block_inverse, block_source, precision=HIGH)


def reference(forcing, slot_wavenumber, inverse, edge_weights):
    degree = jnp.arange(L, dtype=jnp.int32)
    kept_modes = (degree[None, :] >= slot_wavenumber[:, None]).astype(jnp.float32)
    position = jnp.arange(P_SIZE, dtype=jnp.int32)
    interior = ((position > 0) & (position < P_SIZE - 1)).astype(jnp.float32)
    source = forcing.reshape(FIELDS, NSUB, P_SIZE, 2, MTOT, L)
    source = source * kept_modes[None, None, None, None, :, :] * interior[None, None, :, None, None, None]
    source = jnp.transpose(source, (1, 0, 2, 3, 4, 5))
    particular = lax.map(local_solve, (inverse, source))
    low_row = edge_weights[:, 0, :]
    top_row = edge_weights[:, 1, :]
    low_slope = jnp.einsum('sp,sfpcml->sfcml', low_row, particular, precision=HIGH)
    top_slope = jnp.einsum('sp,sfpcml->sfcml', top_row, particular, precision=HIGH)
    lower_unit = inverse[:, :, :, 0, :]
    upper_unit = inverse[:, :, :, P_SIZE - 1, :]
    low_lower = jnp.einsum('sp,sfpl->sfl', low_row, lower_unit, precision=HIGH)
    low_upper = jnp.einsum('sp,sfpl->sfl', low_row, upper_unit, precision=HIGH)
    top_lower = jnp.einsum('sp,sfpl->sfl', top_row, lower_unit, precision=HIGH)
    top_upper = jnp.einsum('sp,sfpl->sfl', top_row, upper_unit, precision=HIGH)
    ratio_now = jnp.zeros((FIELDS, L), jnp.float32)
    reduced = jnp.zeros((FIELDS, 2, MTOT, L), jnp.float32)
    ratio_list = []
    reduced_list = []
    for level in range(NSUB - 1):
        lower_coef = top_lower[level]
        middle_coef = top_upper[level] - low_lower[level + 1]
        upper_coef = -low_upper[level + 1]
        right_side = low_slope[level + 1] - top_slope[level]
        pivot_value = middle_coef - lower_coef * ratio_now
        ratio_now = upper_coef / pivot_value
        reduced = (right_side - lower_coef[:, None, None, :] * reduced) / pivot_value[:, None, None, :]
        ratio_list.append(ratio_now)
        reduced_list.append(reduced)
    later_value = jnp.zeros((FIELDS, 2, MTOT, L), jnp.float32)
    interface = [later_value] * (NSUB - 1)
    for level in range(NSUB - 2, -1, -1):
        later_value = reduced_list[level] - ratio_list[level][:, None, None, :] * later_value
        interface[level] = later_value
    boundary = jnp.zeros((FIELDS, 2, MTOT, L), jnp.float32)
    lower_value = jnp.stack([boundary] + interface)
    upper_value = jnp.stack(interface + [boundary])
    solution = particular + lower_value[:, :, None] * lower_unit[:, :, :, None, None, :]
    solution = solution + upper_value[:, :, None] * upper_unit[:, :, :, None, None, :]
    return jnp.transpose(solution, (1, 0, 2, 3, 4, 5)).reshape(FIELDS, NR, 2, MTOT, L)
```

```python
import functools

import jax
import jax.numpy as jnp
from jax import lax
from jax.experimental import pallas as pl
from jax.experimental.pallas import tpu as pltpu
from jax.sharding import PartitionSpec as P

LANES = 128
ROWS = 8
F32 = jnp.float32
MESH = pl.DeviceIdType.MESH
MARK = 64
VMEM_BYTES = 40 * 1024 * 1024


def grid_iotas():
    row = lax.broadcasted_iota(jnp.int32, (ROWS, LANES), 0)
    lane = lax.broadcasted_iota(jnp.int32, (ROWS, LANES), 1)
    return row, lane


def lane_gather(values, index):
    return jnp.take_along_axis(values, index, axis=1, mode="promise_in_bounds")


def spread(values, k):
    return lane_gather(values, jnp.full((ROWS, LANES), k, jnp.int32))


def exclusive_or(a, b, groups):
    total = 0
    bit = 1
    while bit < groups:
        total = total + lax.rem(a // bit + b // bit, 2) * bit
        bit *= 2
    return total


def pack(pieces, m, degrees):
    _, lane = grid_iotas()
    shift_index = (lane - m) & (LANES - 1)
    left_index = (degrees - 1 - m) & (LANES - 1)
    near, far = pieces[4], pieces[5]
    near_moved = lane_gather(near, shift_index)
    far_moved = lane_gather(far, shift_index)
    first = jnp.where(
        lane >= m, pieces[0], jnp.where(lane - m >= -LANES, far_moved, near_moved)
    )
    second = jnp.where(lane + LANES >= m, pieces[1], far_moved)
    spare = jnp.where(m < LANES, lane_gather(far, left_index), lane_gather(near, left_index))
    return [first, second, pieces[2], pieces[3]], spare


def unpack(pieces, spare, m, degrees):
    _, lane = grid_iotas()
    back_index = (lane + m) & (LANES - 1)
    first = lane_gather(pieces[0], back_index)
    second = lane_gather(pieces[1], back_index)
    moved = [first, jnp.where(lane + m < 2 * LANES, first, second)]
    odd = []
    for t in range(2):
        degree = lane + (2 + t) * LANES
        odd.append(
            jnp.where(
                degree >= degrees - m,
                moved[t],
                jnp.where(degree == degrees - 1 - m, spare, 0.0),
            )
        )
    even = [
        jnp.where(lane >= m, pieces[0], 0.0),
        jnp.where(lane + LANES >= m, pieces[1], 0.0),
        pieces[2],
        pieces[3],
    ]
    return even + odd


def solve_kernel(
    dims, slot, edge, forcing, inverse, landed, values_landed, cols,
    raw, blocks_in, even_src, odd_src, part, weighed, packed, ends, everyone, values,
    raw_sem, in_sem, w_sem, z_send, z_recv, p_send, p_recv, u_send, u_recv, f_send, f_recv,
):
    fields, points, degrees, group, subs, groups = dims
    tiles = degrees // LANES
    half = tiles // 2
    wide = tiles + half
    blocks = points // ROWS
    sub = lax.axis_index("sub")
    me = lax.axis_index("ma")
    row, lane = grid_iotas()
    is_even = (row & 1) == 0
    parity = lax.rem(me, 2)
    pair = me + 1 - 2 * parity

    def other(k):
        return exclusive_or(me, k, groups)

    middle = groups - 4

    def early_mask(i):
        return groups - 2 + i

    def late_mask(j):
        return 2 + (middle // 2) * (1 - lax.rem(j, 2)) + j // 2

    def fetch(k, f):
        return pltpu.make_async_copy(
            inverse.at[0, f, pl.ds(other(k) * group, group)],
            blocks_in.at[k, f],
            in_sem.at[k, f],
        )

    def load(f, h):
        part_q = pl.ds(h * (points // 2), points // 2)
        return pltpu.make_async_copy(forcing.at[f, part_q], raw.at[f, part_q], raw_sem.at[f, h])

    def send(k, f):
        return pltpu.make_async_remote_copy(
            src_ref=packed.at[k, f], dst_ref=landed.at[k, f],
            send_sem=p_send.at[k, f], recv_sem=p_recv.at[k, f],
            device_id=(sub, other(k)), device_id_type=MESH,
        )

    def send_values(k):
        to = pair if k == 0 else other(k)
        return pltpu.make_async_remote_copy(
            src_ref=values, dst_ref=values_landed.at[1 if k == 0 else k],
            send_sem=u_send.at[k // 2], recv_sem=u_recv.at[k // 2],
            device_id=(sub, to), device_id_type=MESH,
        )

    def forward(k):
        return pltpu.make_async_remote_copy(
            src_ref=values_landed.at[k], dst_ref=values_landed.at[k + 1],
            send_sem=f_send.at[k // 2], recv_sem=f_recv.at[k // 2],
            device_id=(sub, pair), device_id_type=MESH,
        )

    load(0, 0).start()
    load(0, 1).start()
    fetch(early_mask(0), 0).start()
    barrier = pltpu.get_barrier_semaphore()
    subs_to = [lax.rem(sub + n, subs) for n in range(1, subs)]
    for to in subs_to:
        pl.semaphore_signal(barrier, inc=1, device_id=(to, me), device_id_type=MESH)
    for k in range(1, groups):
        pl.semaphore_signal(barrier, inc=1, device_id=(sub, other(k)), device_id_type=MESH)

    m = jnp.zeros((ROWS, LANES), jnp.int32)
    for j in range(ROWS // 2):
        m = jnp.where((row >> 1) == j, slot[2 * j], m)

    def prepare(f, h):
        def one(q, _):
            inside = jnp.where((q > 0) & (q < points - 1), 1.0, 0.0).astype(F32)
            for t in range(tiles):
                at = pl.ds(t * LANES, LANES)
                a = raw[f, q, 0, :, at] * inside
                b = raw[f, q, 1, :, at] * inside
                degree = lane + t * LANES
                mixed = jnp.where(is_even, a, pltpu.roll(b, 1, 0))
                even_src[f, q, t] = jnp.where(degree >= m, mixed, 0.0)
                if t >= half:
                    mixed = jnp.where(is_even, pltpu.roll(a, ROWS - 1, 0), b)
                    odd_src[f, q, t - half] = jnp.where(degree >= degrees - 1 - m, mixed, 0.0)
            return 0

        def two(n, _):
            one(2 * n, 0)
            return one(2 * n + 1, 0)

        lax.fori_loop(h * (points // 4), (h + 1) * (points // 4), two, 0)

    def solve_half(k, f, dest):
        left = jnp.where(lane == MARK, m.astype(F32), 0.0)
        for t in range(tiles):
            at = pl.ds(t * LANES, LANES)
            both = t >= half

            def step(n, sums, t=t, at=at, both=both):
                sums = list(sums)
                for b in range(2):
                    block = 2 * n + b
                    for r in range(ROWS):
                        q = block * ROWS + r
                        even = even_src[f, q, t]
                        odd = odd_src[f, q, t - half] if both else None
                        for p in range(group):
                            line = blocks_in[k, f, p, block, pl.ds(r, 1), at]
                            entry = jnp.broadcast_to(line, (ROWS, LANES))
                            sums[p] += entry * even
                            if both:
                                sums[group + p] += entry * odd
                return tuple(sums)

            count = group * (2 if both else 1)
            start = tuple(jnp.zeros((ROWS, LANES), F32) for _ in range(count))
            sums = lax.fori_loop(0, blocks // 2, step, start)
            for p in range(group):
                part[p, t] = sums[p]
                if both:
                    part[p, tiles + t - half] = sums[group + p]
        for p in range(group):
            pieces, spare = pack([part[p, t] for t in range(wide)], m, degrees)
            for t in range(tiles):
                dest[p * tiles + t] = pieces[t]
            left = jnp.where(lane == p, spare, left)
        dest[group * tiles] = left

    load(0, 0).wait()
    first = early_mask(0)
    load(1, 0).start()
    load(1, 1).start()
    fetch(first, 1).start()
    prepare(0, 0)
    load(0, 1).wait()
    fetch(early_mask(1), 0).start()
    fetch(early_mask(1), 1).start()
    prepare(0, 1)
    fetch(first, 0).wait()
    solve_half(first, 0, packed.at[first, 0])
    pl.semaphore_wait(barrier, subs + groups - 2)
    send(first, 0).start()
    load(1, 0).wait()
    load(1, 1).wait()
    for j in range(middle):
        for f in range(fields):
            fetch(late_mask(j), f).start()
    for k in (1, 0):
        for f in range(fields):
            fetch(k, f).start()
    for h in range(2):
        prepare(1, h)

    def early(h, _):
        k, f = early_mask(h // 2), lax.rem(h, 2)
        fetch(k, f).wait()
        solve_half(k, f, packed.at[k, f])
        send(k, f).start()
        return 0

    lax.fori_loop(1, 2 * fields, early, 0)

    def arrive(j, _):
        for f in range(fields):
            fetch(j, f).wait()
        return 0

    lax.fori_loop(0, groups - 2, arrive, 0)

    mine = blocks // 2
    own_blocks = parity * mine

    def weigh(f, _):
        def add(k, sums):
            sums = list(sums)
            for p in range(group):
                low = edge[0, 0, other(k) * group + p]
                top = edge[0, 1, other(k) * group + p]
                for b in range(mine):
                    for t in range(tiles):
                        entry = blocks_in[k, f, p, own_blocks + b, :, pl.ds(t * LANES, LANES)]
                        n = b * tiles + t
                        sums[n] += low * entry
                        sums[mine * tiles + n] += top * entry
            return tuple(sums)

        start = tuple(jnp.zeros((ROWS, LANES), F32) for _ in range(2 * mine * tiles))
        sums = lax.fori_loop(0, groups, add, start)
        for e in range(2):
            for b in range(mine):
                for t in range(tiles):
                    weighed[own_blocks + b, e, f, t] = sums[(e * mine + b) * tiles + t]
        return 0

    lax.fori_loop(0, fields, weigh, 0)
    shared = weighed.at[pl.ds(own_blocks, mine)]
    swap = pltpu.make_async_remote_copy(
        src_ref=shared, dst_ref=shared, send_sem=w_sem.at[0], recv_sem=w_sem.at[1],
        device_id=(sub, pair), device_id_type=MESH,
    )
    swap.start()

    def late(h, _):
        j, f = h // 2, lax.rem(h, 2)
        k = late_mask(j)
        solve_half(k, f, packed.at[k, f])

        @pl.when((f == 0) | (j < middle - 2))
        def _():
            send(k, f).start()

        return 0

    lax.fori_loop(0, 1, late, 0)
    swap.wait()

    slope_tiles = fields * tiles
    lefts = [jnp.zeros((ROWS, LANES), F32) for _ in range(2)]
    for f in range(fields):
        def slope_step(block, sums, f=f):
            sums = list(sums)
            for r in range(ROWS):
                q = block * ROWS + r
                for t in range(tiles):
                    even = even_src[f, q, t]
                    odd = odd_src[f, q, t - half] if t >= half else None
                    for e in range(2):
                        line = weighed[block, e, f, t, pl.ds(r, 1), :]
                        entry = jnp.broadcast_to(line, (ROWS, LANES))
                        sums[e * wide + t] += entry * even
                        if t >= half:
                            sums[e * wide + t + half] += entry * odd
            return tuple(sums)

        start = tuple(jnp.zeros((ROWS, LANES), F32) for _ in range(2 * wide))
        sums = lax.fori_loop(0, blocks, slope_step, start)
        for e in range(2):
            pieces, spare = pack(list(sums[e * wide:(e + 1) * wide]), m, degrees)
            for t in range(tiles):
                ends[e, f * tiles + t] = pieces[t]
            lefts[e] = jnp.where(lane == f, spare, lefts[e])
            for w in range(2):
                for t in range(tiles):
                    line = weighed[w * (blocks - 1), e, f, t, pl.ds(w * (ROWS - 1), 1), :]
                    ends[e, slope_tiles + 1 + t, pl.ds(f * 2 + w, 1), :] = line
    for e in range(2):
        ends[e, slope_tiles] = lefts[e]

    def holds(s, e):
        return s > 0 if e == 0 else s < subs - 1

    def exchange(n, e):
        return pltpu.make_async_remote_copy(
            src_ref=ends.at[e], dst_ref=everyone.at[sub, e],
            send_sem=z_send.at[n, e], recv_sem=z_recv.at[n, e],
            device_id=(subs_to[n], me), device_id_type=MESH,
        )

    for n in range(subs - 1):
        for e in range(2):
            @pl.when(holds(sub, e))
            def _(n=n, e=e):
                exchange(n, e).start()

    everyone[sub] = ends[...]

    lax.fori_loop(1, middle * fields, late, 0)

    def to_pair(f, _):
        solve_half(1, f, packed.at[1, f])
        send(1, f).start()
        return 0

    lax.fori_loop(0, fields, to_pair, 0)

    def to_self(f, _):
        solve_half(0, f, landed.at[0, f])
        return 0

    lax.fori_loop(0, fields, to_self, 0)
    for f in range(fields):
        for p in range(group):
            cols[0, f, pl.ds(p, 1), :] = blocks_in[0, f, p, 0, pl.ds(0, 1), :]
            cols[1, f, pl.ds(p, 1), :] = blocks_in[0, f, p, blocks - 1, pl.ds(ROWS - 1, 1), :]

    for n in range(subs - 1):
        sender = lax.rem(sub + subs - n - 1, subs)
        for e in range(2):
            @pl.when(holds(sub, e))
            def _(n=n, e=e):
                exchange(n, e).wait_send()

            @pl.when(holds(sender, e))
            def _(n=n, e=e):
                exchange(n, e).wait_recv()

    spares = jnp.zeros((ROWS, LANES), F32)
    for f in range(fields):
        def slopes(s, e):
            pieces = [everyone[s, e, f * tiles + t] for t in range(tiles)]
            return unpack(pieces, spread(everyone[s, e, slope_tiles], f), m, degrees)

        rights = []
        for k in range(subs - 1):
            low, top = slopes(k + 1, 0), slopes(k, 1)
            rights.append([low[t] - top[t] for t in range(wide)])
        lower, upper = [], []
        for t in range(wide):
            source = t if t < tiles else t - half

            def influence(s, e, w):
                line = everyone[s, e, slope_tiles + 1 + source, pl.ds(f * 2 + w, 1), :]
                return jnp.broadcast_to(line, (ROWS, LANES))

            zero = jnp.zeros((ROWS, LANES), F32)
            ratio, reduced = zero, zero
            ratios, reduceds = [], []
            for k in range(subs - 1):
                low = influence(k, 1, 0)
                diagonal = influence(k, 1, 1) - influence(k + 1, 0, 0)
                up = -influence(k + 1, 0, 1)
                pivot = diagonal - low * ratio
                reduced = (rights[k][t] - low * reduced) / pivot
                ratio = up / pivot
                ratios.append(ratio)
                reduceds.append(reduced)
            later = zero
            lower_value, upper_value = zero, zero
            for k in range(subs - 2, -1, -1):
                later = reduceds[k] - ratios[k] * later
                lower_value = jnp.where(sub == k + 1, later, lower_value)
                upper_value = jnp.where(sub == k, later, upper_value)
            lower.append(lower_value)
            upper.append(upper_value)
        for e, vector in enumerate((lower, upper)):
            pieces, spare = pack(vector, m, degrees)
            for t in range(tiles):
                values[(e * fields + f) * tiles + t] = pieces[t]
            spares = jnp.where(lane == e * fields + f, spare, spares)
    values[2 * fields * tiles] = spares

    masks = list(range(groups - 2, 0, -2))
    for k in masks + [0]:
        send_values(k).start()
    for j in range(middle - 2, middle):
        send(late_mask(j), 1).start()
    values_landed[0] = values[...]
    for k in masks:
        send_values(k).wait_recv()
        forward(k).start()
    for k in range(1, groups):
        for f in range(fields):
            send(k, f).wait()
    send_values(0).wait()
    for k in masks:
        send_values(k).wait_send()
        forward(k).wait()


def finish_kernel(dims, landed, values, cols, result, out, out_sem):
    fields, degrees, group, groups = dims
    tiles = degrees // LANES
    half = tiles // 2
    wide = tiles + half
    me = lax.axis_index("ma")
    row, lane = grid_iotas()
    is_even = (row & 1) == 0

    def put(k):
        at = exclusive_or(me, k, groups) * ROWS
        rows = pl.ds(pl.multiple_of(at, ROWS), ROWS)
        return pltpu.make_async_copy(out.at[k], result.at[:, :, :, rows, :], out_sem.at[k])

    def one(k, _):
        for f in range(fields):
            left = landed[k, f, group * tiles]
            m = spread(left, MARK).astype(jnp.int32)
            added = []
            for e in range(2):
                n = e * fields + f
                pieces = [values[k, n * tiles + t] for t in range(tiles)]
                spare = spread(values[k, 2 * fields * tiles], n)
                added.append(unpack(pieces, spare, m, degrees))
            for p in range(group):
                pieces = [landed[k, f, p * tiles + t] for t in range(tiles)]
                full = unpack(pieces, spread(left, p), m, degrees)
                for t in range(tiles):
                    at = pl.ds(t * LANES, LANES)
                    low = jnp.broadcast_to(cols[0, f, pl.ds(p, 1), at], (ROWS, LANES))
                    top = jnp.broadcast_to(cols[1, f, pl.ds(p, 1), at], (ROWS, LANES))
                    e = full[t] + added[0][t] * low
                    e = e + added[1][t] * top
                    o = jnp.zeros((ROWS, LANES), F32)
                    if t >= half:
                        spot = tiles + t - half
                        o = full[spot] + added[0][spot] * low
                        o = o + added[1][spot] * top
                    out[k, f, p, 0, :, at] = jnp.where(is_even, e, pltpu.roll(o, 1, 0))
                    out[k, f, p, 1, :, at] = jnp.where(is_even, pltpu.roll(e, ROWS - 1, 0), o)
        put(k).start()
        return 0

    lax.fori_loop(0, groups, one, 0)
    for k in range(groups):
        put(k).wait()


def in_hbm(x):
    return pltpu.with_memory_space_constraint(x, pltpu.HBM)


def body(forcing, slot_wavenumber, inverse, edge_weights):
    fields, points, halves, slots, degrees = forcing.shape
    subs, groups = lax.axis_size("sub"), lax.axis_size("ma")
    group = points // groups
    tiles = degrees // LANES
    half = tiles // 2
    wide = tiles + half
    assert halves == 2 and slots == ROWS and tiles == 4 and fields == 2
    assert groups >= 8 and groups & (groups - 1) == 0 and group < MARK
    count = group * tiles + 1
    end_count = fields * tiles + 1 + tiles
    value_count = 2 * fields * tiles + 1
    shape = jax.ShapeDtypeStruct
    blocks = points // ROWS
    dma = pltpu.SemaphoreType.DMA
    landed, values, cols = pl.pallas_call(
        functools.partial(solve_kernel, (fields, points, degrees, group, subs, groups)),
        in_specs=[
            pl.BlockSpec(memory_space=pltpu.SMEM),
            pl.BlockSpec(memory_space=pltpu.SMEM),
            pl.BlockSpec(memory_space=pltpu.HBM),
            pl.BlockSpec(memory_space=pltpu.HBM),
        ],
        out_specs=[
            pl.BlockSpec(memory_space=pltpu.VMEM),
            pl.BlockSpec(memory_space=pltpu.VMEM),
            pl.BlockSpec(memory_space=pltpu.VMEM),
        ],
        out_shape=[
            shape((groups, fields, count, ROWS, LANES), F32),
            shape((groups, value_count, ROWS, LANES), F32),
            shape((2, fields, group, degrees), F32),
        ],
        scratch_shapes=[
            pltpu.VMEM((fields, points, halves, slots, degrees), F32),
            pltpu.VMEM((groups, fields, group, blocks, ROWS, degrees), F32),
            pltpu.VMEM((fields, points, tiles, ROWS, LANES), F32),
            pltpu.VMEM((fields, points, half, ROWS, LANES), F32),
            pltpu.VMEM((group, wide, ROWS, LANES), F32),
            pltpu.VMEM((blocks, 2, fields, tiles, ROWS, LANES), F32),
            pltpu.VMEM((groups, fields, count, ROWS, LANES), F32),
            pltpu.VMEM((2, end_count, ROWS, LANES), F32),
            pltpu.VMEM((subs, 2, end_count, ROWS, LANES), F32),
            pltpu.VMEM((value_count, ROWS, LANES), F32),
            dma((fields, 2)),
            dma((groups, fields)),
            dma((2,)),
            dma((subs - 1, 2)),
            dma((subs - 1, 2)),
            dma((groups, fields)),
            dma((groups, fields)),
            dma((groups // 2,)),
            dma((groups // 2,)),
            dma((groups // 2,)),
            dma((groups // 2,)),
        ],
        compiler_params=pltpu.CompilerParams(
            collective_id=0, has_side_effects=True, vmem_limit_bytes=VMEM_BYTES
        ),
    )(
        in_hbm(slot_wavenumber),
        in_hbm(edge_weights),
        in_hbm(forcing),
        in_hbm(inverse.reshape(1, fields, points, blocks, ROWS, degrees)),
    )

    return pl.pallas_call(
        functools.partial(finish_kernel, (fields, degrees, group, groups)),
        in_specs=[
            pl.BlockSpec(memory_space=pltpu.VMEM),
            pl.BlockSpec(memory_space=pltpu.VMEM),
            pl.BlockSpec(memory_space=pltpu.VMEM),
        ],
        out_specs=pl.BlockSpec(memory_space=pl.ANY),
        out_shape=shape((fields, group, halves, slots * groups, degrees), F32),
        scratch_shapes=[
            pltpu.VMEM((groups, fields, group, halves, slots, degrees), F32),
            dma((groups,)),
        ],
        compiler_params=pltpu.CompilerParams(vmem_limit_bytes=16 * 1024 * 1024),
    )(landed, values, cols)


def solution(mesh):
    return jax.shard_map(
        body,
        mesh=mesh,
        in_specs=(
            P(None, "sub", None, "ma", None),
            P("ma"),
            P("sub", None, None, None, None),
            P("sub", None, None),
        ),
        out_specs=P(None, ("sub", "ma"), None, None, None),
        check_vma=False,
    )
```

```python
import functools

import jax
import jax.numpy as jnp
from jax import lax
from jax.experimental import pallas as pl
from jax.experimental.pallas import tpu as pltpu
from jax.sharding import PartitionSpec as P

LANES = 128
ROWS = 8
F32 = jnp.float32
MESH = pl.DeviceIdType.MESH
MARK = 64
VMEM_BYTES = 40 * 1024 * 1024


def grid_iotas():
    row = lax.broadcasted_iota(jnp.int32, (ROWS, LANES), 0)
    lane = lax.broadcasted_iota(jnp.int32, (ROWS, LANES), 1)
    return row, lane


def lane_gather(values, index):
    return jnp.take_along_axis(values, index, axis=1, mode="promise_in_bounds")


def spread(values, k):
    return lane_gather(values, jnp.full((ROWS, LANES), k, jnp.int32))


def exclusive_or(a, b, groups):
    total = 0
    bit = 1
    while bit < groups:
        total = total + lax.rem(a // bit + b // bit, 2) * bit
        bit *= 2
    return total


def pack(pieces, m, degrees):
    _, lane = grid_iotas()
    shift_index = (lane - m) & (LANES - 1)
    left_index = (degrees - 1 - m) & (LANES - 1)
    near, far = pieces[4], pieces[5]
    near_moved = lane_gather(near, shift_index)
    far_moved = lane_gather(far, shift_index)
    first = jnp.where(
        lane >= m, pieces[0], jnp.where(lane - m >= -LANES, far_moved, near_moved)
    )
    second = jnp.where(lane + LANES >= m, pieces[1], far_moved)
    spare = jnp.where(m < LANES, lane_gather(far, left_index), lane_gather(near, left_index))
    return [first, second, pieces[2], pieces[3]], spare


def unpack(pieces, spare, m, degrees):
    _, lane = grid_iotas()
    back_index = (lane + m) & (LANES - 1)
    first = lane_gather(pieces[0], back_index)
    second = lane_gather(pieces[1], back_index)
    moved = [first, jnp.where(lane + m < 2 * LANES, first, second)]
    odd = []
    for t in range(2):
        degree = lane + (2 + t) * LANES
        odd.append(
            jnp.where(
                degree >= degrees - m,
                moved[t],
                jnp.where(degree == degrees - 1 - m, spare, 0.0),
            )
        )
    even = [
        jnp.where(lane >= m, pieces[0], 0.0),
        jnp.where(lane + LANES >= m, pieces[1], 0.0),
        pieces[2],
        pieces[3],
    ]
    return even + odd


def solve_kernel(
    dims, slot_in, edge_in, forcing, inverse, landed, values_landed, cols,
    slot, edge, raw, blocks_in, even_src, odd_src, part, stash, weighed, packed, ends, everyone,
    uvals, values,
    small_sem, raw_sem, in_sem, w_sem, z_send, z_recv, p_sem, u_sem, f_sem,
):
    fields, points, degrees, group, subs, groups = dims
    tiles = degrees // LANES
    half = tiles // 2
    wide = tiles + half
    blocks = points // ROWS
    sub = lax.axis_index("sub")
    me = lax.axis_index("ma")
    row, lane = grid_iotas()
    is_even = (row & 1) == 0
    parity = lax.rem(me, 2)
    pair = me + 1 - 2 * parity
    far = groups - 2
    middle = groups - 4
    spot_left, spot_influence = tiles, tiles + 1

    def other(k):
        return exclusive_or(me, k, groups)

    def late_mask(j):
        return 2 + (middle // 2) * (1 - lax.rem(j, 2)) + j // 2

    def fetch(k, f):
        index = 0
        if isinstance(k, int) and k >= far:
            index = k - far + 1
        return pltpu.make_async_copy(
            inverse.at[0, f, pl.ds(other(k) * group, group)],
            blocks_in.at[k, f],
            in_sem.at[index, f],
        )

    def rest_arrives(f):
        most = blocks_in.at[pl.ds(0, far), f]
        pltpu.make_async_copy(most, most, in_sem.at[0, f]).wait()

    def load(f, h):
        part_q = pl.ds(h * (points // 2), points // 2)
        return pltpu.make_async_copy(forcing.at[f, part_q], raw.at[f, part_q], raw_sem.at[f, h])

    def send(k, f):
        return pltpu.make_async_remote_copy(
            src_ref=packed.at[k, f], dst_ref=landed.at[k, f],
            send_sem=p_sem.at[0], recv_sem=p_sem.at[1],
            device_id=(sub, other(k)), device_id_type=MESH,
        )

    def send_values(f):
        return pltpu.make_async_remote_copy(
            src_ref=values.at[f], dst_ref=values_landed.at[0, f],
            send_sem=u_sem.at[0, f], recv_sem=u_sem.at[1, f],
            device_id=(sub, other(far)), device_id_type=MESH,
        )

    def forward(f):
        return pltpu.make_async_remote_copy(
            src_ref=values_landed.at[0, f], dst_ref=values_landed.at[1, f],
            send_sem=f_sem.at[0, f], recv_sem=f_sem.at[1, f],
            device_id=(sub, pair), device_id_type=MESH,
        )

    load(0, 0).start()
    load(0, 1).start()
    fetch(far, 0).start()
    slot_copy = pltpu.make_async_copy(slot_in, slot, small_sem.at[0])
    edge_copy = pltpu.make_async_copy(edge_in, edge, small_sem.at[1])
    slot_copy.start()
    edge_copy.start()
    barrier = pltpu.get_barrier_semaphore()
    subs_to = [lax.rem(sub + n, subs) for n in range(1, subs)]
    for to in subs_to:
        pl.semaphore_signal(barrier, inc=1, device_id=(to, me), device_id_type=MESH)
    for k in range(1, groups):
        pl.semaphore_signal(barrier, inc=1, device_id=(sub, other(k)), device_id_type=MESH)
    fetch(far + 1, 0).start()
    slot_copy.wait()
    edge_copy.wait()

    m = jnp.zeros((ROWS, LANES), jnp.int32)
    for j in range(ROWS // 2):
        m = jnp.where((row >> 1) == j, slot[2 * j], m)

    def prepare(f, h):
        def one(q):
            inside = jnp.where((q > 0) & (q < points - 1), 1.0, 0.0).astype(F32)
            for t in range(tiles):
                at = pl.ds(t * LANES, LANES)
                a = raw[f, q, 0, :, at] * inside
                b = raw[f, q, 1, :, at] * inside
                degree = lane + t * LANES
                mixed = jnp.where(is_even, a, pltpu.roll(b, 1, 0))
                even_src[f, q, t] = jnp.where(degree >= m, mixed, 0.0)
                if t >= half:
                    mixed = jnp.where(is_even, pltpu.roll(a, ROWS - 1, 0), b)
                    odd_src[f, q, t - half] = jnp.where(degree >= degrees - 1 - m, mixed, 0.0)

        def two(n, _):
            one(2 * n)
            one(2 * n + 1)
            return 0

        lax.fori_loop(h * (points // 4), (h + 1) * (points // 4), two, 0)

    def solve_half(k, f, into):
        for t in range(tiles):
            at = pl.ds(t * LANES, LANES)
            both = t >= half

            def step(n, sums, t=t, at=at, both=both):
                sums = list(sums)
                for b in range(2):
                    block = 2 * n + b
                    for r in range(ROWS):
                        q = block * ROWS + r
                        even = even_src[f, q, t]
                        odd = odd_src[f, q, t - half] if both else None
                        for p in range(group):
                            line = blocks_in[k, f, p, block, pl.ds(r, 1), at]
                            entry = jnp.broadcast_to(line, (ROWS, LANES))
                            sums[p] += entry * even
                            if both:
                                sums[group + p] += entry * odd
                return tuple(sums)

            count = group * (2 if both else 1)
            start = tuple(jnp.zeros((ROWS, LANES), F32) for _ in range(count))
            sums = lax.fori_loop(0, blocks // 2, step, start)
            for p in range(group):
                into[p, t] = sums[p]
                if both:
                    into[p, tiles + t - half] = sums[group + p]

    def write_half(k, f, source, dest, fold):
        left = jnp.where(lane == MARK, m.astype(F32), 0.0)
        for p in range(group):
            full = [source[p, t] for t in range(wide)]
            if fold:
                for t in range(tiles):
                    at = pl.ds(t * LANES, LANES)
                    line = blocks_in[k, f, p, 0, pl.ds(0, 1), at]
                    low = jnp.broadcast_to(line, (ROWS, LANES))
                    line = blocks_in[k, f, p, blocks - 1, pl.ds(ROWS - 1, 1), at]
                    top = jnp.broadcast_to(line, (ROWS, LANES))
                    for n in (t,) if t < half else (t, t + half):
                        full[n] = full[n] + uvals[f, 0, n] * low
                        full[n] = full[n] + uvals[f, 1, n] * top
            pieces, spare = pack(full, m, degrees)
            for t in range(tiles):
                dest[p * tiles + t] = pieces[t]
            left = jnp.where(lane == p, spare, left)
        dest[group * tiles] = left

    def early(k, f):
        fetch(k, f).wait()
        solve_half(k, f, part)
        write_half(k, f, part, packed.at[k, f], False)

    mine = blocks // 2
    own_blocks = parity * mine

    def weigh(f):
        def add(k, sums):
            sums = list(sums)
            for p in range(group):
                low = edge[0, 0, other(k) * group + p]
                top = edge[0, 1, other(k) * group + p]
                for b in range(mine):
                    for t in range(tiles):
                        entry = blocks_in[k, f, p, own_blocks + b, :, pl.ds(t * LANES, LANES)]
                        n = b * tiles + t
                        sums[n] += low * entry
                        sums[mine * tiles + n] += top * entry
            return tuple(sums)

        start = tuple(jnp.zeros((ROWS, LANES), F32) for _ in range(2 * mine * tiles))
        sums = lax.fori_loop(0, groups, add, start)
        for e in range(2):
            for b in range(mine):
                for t in range(tiles):
                    weighed[f, own_blocks + b, e, t] = sums[(e * mine + b) * tiles + t]

    def swap(f):
        shared = weighed.at[f, pl.ds(own_blocks, mine)]
        return pltpu.make_async_remote_copy(
            src_ref=shared, dst_ref=shared, send_sem=w_sem.at[0, f], recv_sem=w_sem.at[1, f],
            device_id=(sub, pair), device_id_type=MESH,
        )

    def exchange(n, f, sender, begin):
        outer = (sender == 0) | (sender == subs - 1)
        first = 1 - lax.min(sender, 1)
        for count, case in ((1, outer), (2, jnp.logical_not(outer))):
            kept = pl.ds(first, count) if count == 1 else pl.ds(0, 2)
            copy = pltpu.make_async_remote_copy(
                src_ref=ends.at[f, kept], dst_ref=everyone.at[sender, f, kept],
                send_sem=z_send.at[n, f], recv_sem=z_recv.at[n, f],
                device_id=(subs_to[n], me), device_id_type=MESH,
            )

            @pl.when(case)
            def _(copy=copy):
                begin(copy)

    def slopes(f):
        def slope_step(block, sums):
            sums = list(sums)
            for r in range(ROWS):
                q = block * ROWS + r
                for t in range(tiles):
                    even = even_src[f, q, t]
                    odd = odd_src[f, q, t - half] if t >= half else None
                    for e in range(2):
                        line = weighed[f, block, e, t, pl.ds(r, 1), :]
                        entry = jnp.broadcast_to(line, (ROWS, LANES))
                        sums[e * wide + t] += entry * even
                        if t >= half:
                            sums[e * wide + t + half] += entry * odd
            return tuple(sums)

        start = tuple(jnp.zeros((ROWS, LANES), F32) for _ in range(2 * wide))
        sums = lax.fori_loop(0, blocks, slope_step, start)
        for e in range(2):
            pieces, spare = pack(list(sums[e * wide:(e + 1) * wide]), m, degrees)
            for t in range(tiles):
                ends[f, e, t] = pieces[t]
            ends[f, e, spot_left] = spare
            for w in range(2):
                for t in range(tiles):
                    line = weighed[f, w * (blocks - 1), e, t, pl.ds(w * (ROWS - 1), 1), :]
                    ends[f, e, spot_influence, pl.ds(2 * t + w, 1), :] = line
        for n in range(subs - 1):
            exchange(n, f, sub, lambda copy: copy.start())
        everyone[sub, f] = ends[f]

    def interface(f):
        for n in range(subs - 1):
            exchange(n, f, sub, lambda copy: copy.wait_send())
            sender = lax.rem(sub + subs - n - 1, subs)
            exchange(n, f, sender, lambda copy: copy.wait_recv())

        def slopes_of(s, e):
            pieces = [everyone[s, f, e, t] for t in range(tiles)]
            return unpack(pieces, everyone[s, f, e, spot_left], m, degrees)

        rights = []
        for k in range(subs - 1):
            low, top = slopes_of(k + 1, 0), slopes_of(k, 1)
            rights.append([low[t] - top[t] for t in range(wide)])
        lower, upper = [], []
        for t in range(wide):
            source = t if t < tiles else t - half

            def influence(s, e, w):
                line = everyone[s, f, e, spot_influence, pl.ds(2 * source + w, 1), :]
                return jnp.broadcast_to(line, (ROWS, LANES))

            zero = jnp.zeros((ROWS, LANES), F32)
            ratio, reduced = zero, zero
            ratios, reduceds = [], []
            for k in range(subs - 1):
                low = influence(k, 1, 0)
                diagonal = influence(k, 1, 1) - influence(k + 1, 0, 0)
                up = -influence(k + 1, 0, 1)
                pivot = diagonal - low * ratio
                reduced = (rights[k][t] - low * reduced) / pivot
                ratio = up / pivot
                ratios.append(ratio)
                reduceds.append(reduced)
            later = zero
            lower_value, upper_value = zero, zero
            for k in range(subs - 2, -1, -1):
                later = reduceds[k] - ratios[k] * later
                lower_value = jnp.where(sub == k + 1, later, lower_value)
                upper_value = jnp.where(sub == k, later, upper_value)
            lower.append(lower_value)
            upper.append(upper_value)
        spares = jnp.zeros((ROWS, LANES), F32)
        for e, vector in enumerate((lower, upper)):
            for t in range(wide):
                uvals[f, e, t] = vector[t]
            pieces, spare = pack(vector, m, degrees)
            for t in range(tiles):
                values[f, e * tiles + t] = pieces[t]
            spares = jnp.where(lane == e, spare, spares)
        values[f, 2 * tiles] = spares
        send_values(f).start()

    def late_parts(j, f):
        solve_half(late_mask(j), f, stash.at[j])

    def late_write(f):
        def one(j, _):
            k = late_mask(j)
            write_half(k, f, stash.at[j], packed.at[k, f], True)
            send(k, f).start()
            return 0

        lax.fori_loop(0, middle, one, 0)

    load(0, 0).wait()
    load(1, 0).start()
    load(1, 1).start()
    prepare(0, 0)
    load(0, 1).wait()
    for k in range(far):
        fetch(k, 0).start()
    prepare(0, 1)
    early(far, 0)
    for k in (far, far + 1):
        fetch(k, 1).start()
    pl.semaphore_wait(barrier, subs + groups - 2)
    send(far, 0).start()
    for k in range(far):
        fetch(k, 1).start()
    early(far + 1, 0)
    send(far + 1, 0).start()
    rest_arrives(0)
    weigh(0)
    swap(0).start()
    for h in range(2):
        load(1, h).wait()
        prepare(1, h)
    early(far, 1)
    send(far, 1).start()
    swap(0).wait()
    slopes(0)
    early(far + 1, 1)
    send(far + 1, 1).start()
    rest_arrives(1)
    weigh(1)
    swap(1).start()
    late_parts(0, 0)
    swap(1).wait()
    slopes(1)

    def more(f):
        def one(j, _):
            late_parts(j, f)
            return 0

        lax.fori_loop(1 - f, middle, one, 0)

    def turn(f, _):
        more(f)
        interface(f)
        late_write(f)
        return 0

    lax.fori_loop(0, fields, turn, 0)

    def to_pair(f, _):
        solve_half(1, f, part)
        write_half(1, f, part, packed.at[1, f], True)
        send(1, f).start()
        return 0

    lax.fori_loop(0, fields, to_pair, 0)
    for f in range(fields):
        send_values(f).wait_recv()
        forward(f).start()

    def to_self(f, _):
        solve_half(0, f, part)
        write_half(0, f, part, landed.at[0, f], True)
        return 0

    lax.fori_loop(0, fields, to_self, 0)
    for f in range(fields):
        for p in range(group):
            cols[0, f, pl.ds(p, 1), :] = blocks_in[0, f, p, 0, pl.ds(0, 1), :]
            cols[1, f, pl.ds(p, 1), :] = blocks_in[0, f, p, blocks - 1, pl.ds(ROWS - 1, 1), :]
    for f in range(fields):
        send_values(f).wait_send()
        forward(f).wait()
    away = pl.ds(1, groups - 1)
    pltpu.make_async_remote_copy(
        src_ref=packed.at[away], dst_ref=landed.at[away],
        send_sem=p_sem.at[0], recv_sem=p_sem.at[1],
        device_id=(sub, pair), device_id_type=MESH,
    ).wait()


def finish_kernel(dims, landed, values, cols, result, out, out_sem):
    fields, degrees, group, groups = dims
    tiles = degrees // LANES
    half = tiles // 2
    me = lax.axis_index("ma")
    row, _ = grid_iotas()
    is_even = (row & 1) == 0
    far = groups - 2

    def put(k):
        at = exclusive_or(me, k, groups) * ROWS
        rows = pl.ds(pl.multiple_of(at, ROWS), ROWS)
        return pltpu.make_async_copy(out.at[k], result.at[:, :, :, rows, :], out_sem.at[k])

    def one(k, fold):
        for f in range(fields):
            left = landed[k, f, group * tiles]
            m = spread(left, MARK).astype(jnp.int32)
            added = []
            for e in range(2 if fold else 0):
                pieces = [values[k - far, f, e * tiles + t] for t in range(tiles)]
                spare = spread(values[k - far, f, 2 * tiles], e)
                added.append(unpack(pieces, spare, m, degrees))
            for p in range(group):
                pieces = [landed[k, f, p * tiles + t] for t in range(tiles)]
                full = unpack(pieces, spread(left, p), m, degrees)
                for t in range(tiles):
                    at = pl.ds(t * LANES, LANES)
                    spots = (t,) if t < half else (t, t + half)
                    if fold:
                        low = jnp.broadcast_to(cols[0, f, pl.ds(p, 1), at], (ROWS, LANES))
                        top = jnp.broadcast_to(cols[1, f, pl.ds(p, 1), at], (ROWS, LANES))
                        for n in spots:
                            full[n] = full[n] + added[0][n] * low
                            full[n] = full[n] + added[1][n] * top
                    e = full[t]
                    o = full[t + half] if t >= half else jnp.zeros((ROWS, LANES), F32)
                    out[k, f, p, 0, :, at] = jnp.where(is_even, e, pltpu.roll(o, 1, 0))
                    out[k, f, p, 1, :, at] = jnp.where(is_even, pltpu.roll(e, ROWS - 1, 0), o)
        put(k).start()

    def plain(k, _):
        one(k, False)
        return 0

    def folded(k, _):
        one(k, True)
        return 0

    lax.fori_loop(0, far, plain, 0)
    lax.fori_loop(far, groups, folded, 0)
    for k in range(groups):
        put(k).wait()


def in_hbm(x):
    return pltpu.with_memory_space_constraint(x, pltpu.HBM)


def body(forcing, slot_wavenumber, inverse, edge_weights):
    fields, points, halves, slots, degrees = forcing.shape
    subs, groups = lax.axis_size("sub"), lax.axis_size("ma")
    group = points // groups
    tiles = degrees // LANES
    half = tiles // 2
    wide = tiles + half
    assert halves == 2 and slots == ROWS and tiles == 4 and fields == 2
    assert groups >= 8 and groups & (groups - 1) == 0 and group < MARK
    count = group * tiles + 1
    end_count = tiles + 2
    value_count = 2 * tiles + 1
    shape = jax.ShapeDtypeStruct
    blocks = points // ROWS
    dma = pltpu.SemaphoreType.DMA
    landed, values, cols = pl.pallas_call(
        functools.partial(solve_kernel, (fields, points, degrees, group, subs, groups)),
        in_specs=[pl.BlockSpec(memory_space=pltpu.HBM)] * 4,
        out_specs=[pl.BlockSpec(memory_space=pltpu.VMEM)] * 3,
        out_shape=[
            shape((groups, fields, count, ROWS, LANES), F32),
            shape((2, fields, value_count, ROWS, LANES), F32),
            shape((2, fields, group, degrees), F32),
        ],
        scratch_shapes=[
            pltpu.SMEM(slot_wavenumber.shape, slot_wavenumber.dtype),
            pltpu.SMEM(edge_weights.shape, F32),
            pltpu.VMEM((fields, points, halves, slots, degrees), F32),
            pltpu.VMEM((groups, fields, group, blocks, ROWS, degrees), F32),
            pltpu.VMEM((fields, points, tiles, ROWS, LANES), F32),
            pltpu.VMEM((fields, points, half, ROWS, LANES), F32),
            pltpu.VMEM((group, wide, ROWS, LANES), F32),
            pltpu.VMEM((groups - 4, group, wide, ROWS, LANES), F32),
            pltpu.VMEM((fields, blocks, 2, tiles, ROWS, LANES), F32),
            pltpu.VMEM((groups, fields, count, ROWS, LANES), F32),
            pltpu.VMEM((fields, 2, end_count, ROWS, LANES), F32),
            pltpu.VMEM((subs, fields, 2, end_count, ROWS, LANES), F32),
            pltpu.VMEM((fields, 2, wide, ROWS, LANES), F32),
            pltpu.VMEM((fields, value_count, ROWS, LANES), F32),
            dma((2,)),
            dma((fields, 2)),
            dma((3, fields)),
            dma((2, fields)),
            dma((subs - 1, fields)),
            dma((subs - 1, fields)),
            dma((2,)),
            dma((2, fields)),
            dma((2, fields)),
        ],
        compiler_params=pltpu.CompilerParams(
            collective_id=0, has_side_effects=True, vmem_limit_bytes=VMEM_BYTES
        ),
    )(
        in_hbm(slot_wavenumber),
        in_hbm(edge_weights),
        in_hbm(forcing),
        in_hbm(inverse.reshape(1, fields, points, blocks, ROWS, degrees)),
    )

    return pl.pallas_call(
        functools.partial(finish_kernel, (fields, degrees, group, groups)),
        in_specs=[
            pl.BlockSpec(memory_space=pltpu.VMEM),
            pl.BlockSpec(memory_space=pltpu.VMEM),
            pl.BlockSpec(memory_space=pltpu.VMEM),
        ],
        out_specs=pl.BlockSpec(memory_space=pl.ANY),
        out_shape=shape((fields, group, halves, slots * groups, degrees), F32),
        scratch_shapes=[
            pltpu.VMEM((groups, fields, group, halves, slots, degrees), F32),
            dma((groups,)),
        ],
        compiler_params=pltpu.CompilerParams(vmem_limit_bytes=16 * 1024 * 1024),
    )(landed, values, cols)


def solution(mesh):
    return jax.shard_map(
        body,
        mesh=mesh,
        in_specs=(
            P(None, "sub", None, "ma", None),
            P("ma"),
            P("sub", None, None, None, None),
            P("sub", None, None),
        ),
        out_specs=P(None, ("sub", "ma"), None, None, None),
        check_vma=False,
    )
```

```python
import functools

import jax
import jax.numpy as jnp
from jax import lax
from jax.experimental import pallas as pl
from jax.experimental.pallas import tpu as pltpu
from jax.sharding import PartitionSpec as P

LANES = 128
ROWS = 8
F32 = jnp.float32
MESH = pl.DeviceIdType.MESH
MARK = 64
VMEM_BYTES = 40 * 1024 * 1024


def grid_iotas():
    row = lax.broadcasted_iota(jnp.int32, (ROWS, LANES), 0)
    lane = lax.broadcasted_iota(jnp.int32, (ROWS, LANES), 1)
    return row, lane


def lane_gather(values, index):
    return jnp.take_along_axis(values, index, axis=1, mode="promise_in_bounds")


def spread(values, k):
    return lane_gather(values, jnp.full((ROWS, LANES), k, jnp.int32))


def exclusive_or(a, b, groups):
    total = 0
    bit = 1
    while bit < groups:
        total = total + lax.rem(a // bit + b // bit, 2) * bit
        bit *= 2
    return total


def pack(pieces, m, degrees):
    _, lane = grid_iotas()
    shift_index = (lane - m) & (LANES - 1)
    left_index = (degrees - 1 - m) & (LANES - 1)
    near, far = pieces[4], pieces[5]
    near_moved = lane_gather(near, shift_index)
    far_moved = lane_gather(far, shift_index)
    first = jnp.where(
        lane >= m, pieces[0], jnp.where(lane - m >= -LANES, far_moved, near_moved)
    )
    second = jnp.where(lane + LANES >= m, pieces[1], far_moved)
    spare = jnp.where(m < LANES, lane_gather(far, left_index), lane_gather(near, left_index))
    return [first, second, pieces[2], pieces[3]], spare


def unpack(pieces, spare, m, degrees):
    _, lane = grid_iotas()
    back_index = (lane + m) & (LANES - 1)
    first = lane_gather(pieces[0], back_index)
    second = lane_gather(pieces[1], back_index)
    moved = [first, jnp.where(lane + m < 2 * LANES, first, second)]
    odd = []
    for t in range(2):
        degree = lane + (2 + t) * LANES
        odd.append(
            jnp.where(
                degree >= degrees - m,
                moved[t],
                jnp.where(degree == degrees - 1 - m, spare, 0.0),
            )
        )
    even = [
        jnp.where(lane >= m, pieces[0], 0.0),
        jnp.where(lane + LANES >= m, pieces[1], 0.0),
        pieces[2],
        pieces[3],
    ]
    return even + odd


def solve_kernel(
    dims, slot_in, edge_in, forcing, inverse, landed, values_landed, cols,
    slot, edge, raw, blocks_in, even_src, odd_src, part, stash, weighed, packed, lefts, ends,
    everyone, uvals, values,
    small_sem, raw_sem, in_sem, w_sem, z_send, z_recv, p_sem, u_sem, f_sem,
):
    fields, points, degrees, group, subs, groups = dims
    tiles = degrees // LANES
    half = tiles // 2
    wide = tiles + half
    blocks = points // ROWS
    sub = lax.axis_index("sub")
    me = lax.axis_index("ma")
    row, lane = grid_iotas()
    is_even = (row & 1) == 0
    parity = lax.rem(me, 2)
    pair = me + 1 - 2 * parity
    far = groups - 2
    middle = groups - 4
    size = group * tiles
    mine = blocks // 2
    own_blocks = pl.ds(parity * mine, mine)
    its_blocks = pl.ds((1 - parity) * mine, mine)
    spot_left, spot_influence = tiles, tiles + 1

    def other(k):
        return exclusive_or(me, k, groups)

    def late_mask(j):
        return 2 + (middle // 2) * (1 - lax.rem(j, 2)) + j // 2

    def fetch(k, f, which, n):
        return pltpu.make_async_copy(
            inverse.at[0, f, pl.ds(other(k) * group, group), which],
            blocks_in.at[k, f, :, which],
            in_sem.at[n],
        )

    def arrived(count, f, which, n):
        target = blocks_in.at[pl.ds(0, count), f, :, which]
        pltpu.make_async_copy(target, target, in_sem.at[n]).wait()

    everything = pl.ds(0, blocks)

    def load(f, h):
        part_q = pl.ds(h * (points // 2), points // 2)
        return pltpu.make_async_copy(forcing.at[f, part_q], raw.at[f, part_q], raw_sem.at[f, h])

    def send(k, f, begin=0, end=None):
        if end is None:
            end = size + (f == fields - 1)
        rows = pl.ds(f * size + begin, end - begin)
        return pltpu.make_async_remote_copy(
            src_ref=packed.at[k, rows], dst_ref=landed.at[k, rows],
            send_sem=p_sem.at[0], recv_sem=p_sem.at[1],
            device_id=(sub, other(k)), device_id_type=MESH,
        )

    def value_rows(f):
        return pl.ds(f * 2 * tiles, 2 * tiles + (f == fields - 1))

    def send_values(f):
        return pltpu.make_async_remote_copy(
            src_ref=values.at[value_rows(f)], dst_ref=values_landed.at[0, value_rows(f)],
            send_sem=u_sem.at[0, f], recv_sem=u_sem.at[1, f],
            device_id=(sub, other(far)), device_id_type=MESH,
        )

    def forward(f):
        return pltpu.make_async_remote_copy(
            src_ref=values_landed.at[0, value_rows(f)], dst_ref=values_landed.at[1, value_rows(f)],
            send_sem=f_sem.at[0, f], recv_sem=f_sem.at[1, f],
            device_id=(sub, pair), device_id_type=MESH,
        )

    load(0, 0).start()
    load(0, 1).start()
    fetch(far + 1, 0, everything, 0).start()
    slot_copy = pltpu.make_async_copy(slot_in, slot, small_sem.at[0])
    edge_copy = pltpu.make_async_copy(edge_in, edge, small_sem.at[1])
    slot_copy.start()
    edge_copy.start()
    barrier = pltpu.get_barrier_semaphore()
    subs_to = [lax.rem(sub + n, subs) for n in range(1, subs)]
    for to in subs_to:
        pl.semaphore_signal(barrier, inc=1, device_id=(to, me), device_id_type=MESH)
    for k in range(1, groups):
        pl.semaphore_signal(barrier, inc=1, device_id=(sub, other(k)), device_id_type=MESH)
    slot_copy.wait()
    edge_copy.wait()

    m = jnp.zeros((ROWS, LANES), jnp.int32)
    for j in range(ROWS // 2):
        m = jnp.where((row >> 1) == j, slot[2 * j], m)

    def prepare(f, h):
        def one(q):
            inside = jnp.where((q > 0) & (q < points - 1), 1.0, 0.0).astype(F32)
            for t in range(tiles):
                at = pl.ds(t * LANES, LANES)
                a = raw[f, q, 0, :, at] * inside
                b = raw[f, q, 1, :, at] * inside
                degree = lane + t * LANES
                mixed = jnp.where(is_even, a, pltpu.roll(b, 1, 0))
                even_src[f, q, t] = jnp.where(degree >= m, mixed, 0.0)
                if t >= half:
                    mixed = jnp.where(is_even, pltpu.roll(a, ROWS - 1, 0), b)
                    odd_src[f, q, t - half] = jnp.where(degree >= degrees - 1 - m, mixed, 0.0)

        def two(n, _):
            one(2 * n)
            one(2 * n + 1)
            return 0

        lax.fori_loop(h * (points // 4), (h + 1) * (points // 4), two, 0)

    def solve_half(k, f, into, begin=0, end=group):
        for span in (tuple(range(half)),) + tuple((t,) for t in range(half, tiles)):
            units = [(p, t, 0) for t in span for p in range(begin, end)]
            if span[0] >= half:
                units += [(p, t, 1) for t in span for p in range(begin, end)]

            def step(n, sums, span=span, units=units):
                sums = dict(zip(units, sums))
                for b in range(2):
                    block = 2 * n + b
                    for r in range(ROWS):
                        q = block * ROWS + r
                        for t in span:
                            even = even_src[f, q, t]
                            odd = odd_src[f, q, t - half] if t >= half else None
                            for p in range(begin, end):
                                line = blocks_in[
                                    k, f, p, block, pl.ds(r, 1), pl.ds(t * LANES, LANES)
                                ]
                                entry = jnp.broadcast_to(line, (ROWS, LANES))
                                sums[p, t, 0] += entry * even
                                if t >= half:
                                    sums[p, t, 1] += entry * odd
                return tuple(sums[unit] for unit in units)

            start = tuple(jnp.zeros((ROWS, LANES), F32) for _ in units)
            sums = lax.fori_loop(0, blocks // 2, step, start)
            for (p, t, o), total in zip(units, sums):
                into[p, t + half * o] = total

    def write_half(k, f, source, dest, fold, begin=0, end=group):
        if f == 0 and begin == 0:
            left = jnp.where(lane == MARK, m.astype(F32), 0.0)
        else:
            left = lefts[k]
        for p in range(begin, end):
            full = [source[p, t] for t in range(wide)]
            if fold:
                for t in range(tiles):
                    at = pl.ds(t * LANES, LANES)
                    line = blocks_in[k, f, p, 0, pl.ds(0, 1), at]
                    low = jnp.broadcast_to(line, (ROWS, LANES))
                    line = blocks_in[k, f, p, blocks - 1, pl.ds(ROWS - 1, 1), at]
                    top = jnp.broadcast_to(line, (ROWS, LANES))
                    for n in (t,) if t < half else (t, t + half):
                        full[n] = full[n] + uvals[f, 0, n] * low
                        full[n] = full[n] + uvals[f, 1, n] * top
            pieces, spare = pack(full, m, degrees)
            for t in range(tiles):
                dest[f * size + p * tiles + t] = pieces[t]
            left = jnp.where(lane == f * group + p, spare, left)
        if f == fields - 1 and end == group:
            dest[fields * size] = left
        else:
            lefts[k] = left

    def early(k, f):
        solve_half(k, f, part)
        write_half(k, f, part, packed.at[k], False)
        send(k, f).start()

    def weigh(f):
        def add(k, sums):
            sums = list(sums)
            for p in range(group):
                low = edge[0, 0, other(k) * group + p]
                top = edge[0, 1, other(k) * group + p]
                for b in range(mine):
                    for t in range(tiles):
                        at = parity * mine + b
                        entry = blocks_in[k, f, p, at, :, pl.ds(t * LANES, LANES)]
                        n = b * tiles + t
                        sums[n] += low * entry
                        sums[mine * tiles + n] += top * entry
            return tuple(sums)

        start = tuple(jnp.zeros((ROWS, LANES), F32) for _ in range(2 * mine * tiles))
        sums = lax.fori_loop(0, groups, add, start)
        for e in range(2):
            for b in range(mine):
                for t in range(tiles):
                    weighed[f, parity * mine + b, e, t] = sums[(e * mine + b) * tiles + t]

    def swap(f):
        shared = weighed.at[f, own_blocks]
        return pltpu.make_async_remote_copy(
            src_ref=shared, dst_ref=shared, send_sem=w_sem.at[0, f], recv_sem=w_sem.at[1, f],
            device_id=(sub, pair), device_id_type=MESH,
        )

    def exchange(n, f, sender, begin):
        outer = (sender == 0) | (sender == subs - 1)
        first = 1 - lax.min(sender, 1)
        for count, case in ((1, outer), (2, jnp.logical_not(outer))):
            kept = pl.ds(first, count) if count == 1 else pl.ds(0, 2)
            copy = pltpu.make_async_remote_copy(
                src_ref=ends.at[f, kept], dst_ref=everyone.at[sender, f, kept],
                send_sem=z_send.at[n, f], recv_sem=z_recv.at[n, f],
                device_id=(subs_to[n], me), device_id_type=MESH,
            )

            @pl.when(case)
            def _(copy=copy):
                begin(copy)

    def slopes(f):
        def slope_step(block, sums):
            sums = list(sums)
            for r in range(ROWS):
                q = block * ROWS + r
                for t in range(tiles):
                    even = even_src[f, q, t]
                    odd = odd_src[f, q, t - half] if t >= half else None
                    for e in range(2):
                        line = weighed[f, block, e, t, pl.ds(r, 1), :]
                        entry = jnp.broadcast_to(line, (ROWS, LANES))
                        sums[e * wide + t] += entry * even
                        if t >= half:
                            sums[e * wide + t + half] += entry * odd
            return tuple(sums)

        start = tuple(jnp.zeros((ROWS, LANES), F32) for _ in range(2 * wide))
        sums = lax.fori_loop(0, blocks, slope_step, start)
        for e in range(2):
            pieces, spare = pack(list(sums[e * wide:(e + 1) * wide]), m, degrees)
            for t in range(tiles):
                ends[f, e, t] = pieces[t]
            ends[f, e, spot_left] = spare
            for w in range(2):
                for t in range(tiles):
                    line = weighed[f, w * (blocks - 1), e, t, pl.ds(w * (ROWS - 1), 1), :]
                    ends[f, e, spot_influence, pl.ds(2 * t + w, 1), :] = line
        for n in range(subs - 1):
            exchange(n, f, sub, lambda copy: copy.start())
        everyone[sub, f] = ends[f]

    def interface(f):
        for n in range(subs - 1):
            exchange(n, f, sub, lambda copy: copy.wait_send())
            sender = lax.rem(sub + subs - n - 1, subs)
            exchange(n, f, sender, lambda copy: copy.wait_recv())

        def slopes_of(s, e):
            pieces = [everyone[s, f, e, t] for t in range(tiles)]
            return unpack(pieces, everyone[s, f, e, spot_left], m, degrees)

        rights = []
        for k in range(subs - 1):
            low, top = slopes_of(k + 1, 0), slopes_of(k, 1)
            rights.append([low[t] - top[t] for t in range(wide)])
        lower, upper = [], []
        for t in range(wide):
            source = t if t < tiles else t - half

            def influence(s, e, w):
                line = everyone[s, f, e, spot_influence, pl.ds(2 * source + w, 1), :]
                return jnp.broadcast_to(line, (ROWS, LANES))

            zero = jnp.zeros((ROWS, LANES), F32)
            ratio, reduced = zero, zero
            ratios, reduceds = [], []
            for k in range(subs - 1):
                low = influence(k, 1, 0)
                diagonal = influence(k, 1, 1) - influence(k + 1, 0, 0)
                up = -influence(k + 1, 0, 1)
                pivot = diagonal - low * ratio
                reduced = (rights[k][t] - low * reduced) / pivot
                ratio = up / pivot
                ratios.append(ratio)
                reduceds.append(reduced)
            later = zero
            lower_value, upper_value = zero, zero
            for k in range(subs - 2, -1, -1):
                later = reduceds[k] - ratios[k] * later
                lower_value = jnp.where(sub == k + 1, later, lower_value)
                upper_value = jnp.where(sub == k, later, upper_value)
            lower.append(lower_value)
            upper.append(upper_value)
        spares = values[fields * 2 * tiles] if f else jnp.zeros((ROWS, LANES), F32)
        for e, vector in enumerate((lower, upper)):
            for t in range(wide):
                uvals[f, e, t] = vector[t]
            pieces, spare = pack(vector, m, degrees)
            for t in range(tiles):
                values[f * 2 * tiles + e * tiles + t] = pieces[t]
            spares = jnp.where(lane == 2 * f + e, spare, spares)
        values[fields * 2 * tiles] = spares
        send_values(f).start()

    def late_parts(j, f):
        solve_half(late_mask(j), f, stash.at[j])

    def late_write(f):
        def one(j, _):
            k = late_mask(j)
            write_half(k, f, stash.at[j], packed.at[k], True)
            send(k, f).start()
            return 0

        lax.fori_loop(0, middle, one, 0)

    load(0, 0).wait()
    for k in range(far + 1):
        fetch(k, 0, own_blocks, 1).start()
    prepare(0, 0)
    load(0, 1).wait()
    fetch(far, 0, its_blocks, 2).start()
    prepare(0, 1)
    fetch(far + 1, 0, everything, 0).wait()
    for k in range(far):
        fetch(k, 0, its_blocks, 3).start()
    for h in range(2):
        load(1, h).start()
    quarter = group // 2
    solve_half(far + 1, 0, part, 0, quarter)
    write_half(far + 1, 0, part, packed.at[far + 1], False, 0, quarter)
    pl.semaphore_wait(barrier, subs + groups - 2)
    send(far + 1, 0, 0, quarter * tiles).start()
    for k in (far + 1, far):
        fetch(k, 1, everything, 4 + far + 1 - k).start()
    solve_half(far + 1, 0, part, quarter, group)
    write_half(far + 1, 0, part, packed.at[far + 1], False, quarter, group)
    send(far + 1, 0, quarter * tiles).start()
    arrived(far + 1, 0, own_blocks, 1)
    for k in range(far):
        fetch(k, 1, everything, 6).start()
    weigh(0)
    swap(0).start()
    fetch(far, 0, its_blocks, 2).wait()
    early(far, 0)
    swap(0).wait()
    slopes(0)
    for h in range(2):
        load(1, h).wait()
        prepare(1, h)
    fetch(far + 1, 1, everything, 4).wait()
    early(far + 1, 1)
    fetch(far, 1, everything, 5).wait()
    early(far, 1)
    arrived(far, 0, its_blocks, 3)
    arrived(far, 1, everything, 6)
    weigh(1)
    swap(1).start()
    late_parts(0, 0)
    swap(1).wait()
    slopes(1)
    for f in range(fields):
        def more(j, _, f=f):
            late_parts(j, f)
            return 0

        lax.fori_loop(1 if f == 0 else 0, middle, more, 0)
        interface(f)
        late_write(f)

    for f in range(fields):
        solve_half(1, f, part)
        write_half(1, f, part, packed.at[1], True)
        send(1, f).start()
    for f in range(fields):
        send_values(f).wait_recv()
        forward(f).start()
    for f in range(fields):
        solve_half(0, f, part)
        write_half(0, f, part, landed.at[0], True)
    for f in range(fields):
        for p in range(group):
            cols[0, f, pl.ds(p, 1), :] = blocks_in[0, f, p, 0, pl.ds(0, 1), :]
            cols[1, f, pl.ds(p, 1), :] = blocks_in[0, f, p, blocks - 1, pl.ds(ROWS - 1, 1), :]
    for f in range(fields):
        send_values(f).wait_send()
        forward(f).wait()
    away = pl.ds(1, groups - 1)
    pltpu.make_async_remote_copy(
        src_ref=packed.at[away], dst_ref=landed.at[away],
        send_sem=p_sem.at[0], recv_sem=p_sem.at[1],
        device_id=(sub, pair), device_id_type=MESH,
    ).wait()


def finish_kernel(dims, landed, values, cols, result, out, out_sem):
    fields, degrees, group, groups = dims
    tiles = degrees // LANES
    half = tiles // 2
    me = lax.axis_index("ma")
    row, _ = grid_iotas()
    is_even = (row & 1) == 0
    far = groups - 2

    def put(k):
        at = exclusive_or(me, k, groups) * ROWS
        rows = pl.ds(pl.multiple_of(at, ROWS), ROWS)
        return pltpu.make_async_copy(out.at[k], result.at[:, :, :, rows, :], out_sem.at[k])

    def one(k, fold):
        left = landed[k, fields * group * tiles]
        m = spread(left, MARK).astype(jnp.int32)
        for f in range(fields):
            added = []
            for e in range(2 if fold else 0):
                at = (2 * f + e) * tiles
                pieces = [values[k - far, at + t] for t in range(tiles)]
                spare = spread(values[k - far, fields * 2 * tiles], 2 * f + e)
                added.append(unpack(pieces, spare, m, degrees))
            for p in range(group):
                n = f * group + p
                pieces = [landed[k, n * tiles + t] for t in range(tiles)]
                full = unpack(pieces, spread(left, n), m, degrees)
                for t in range(tiles):
                    at = pl.ds(t * LANES, LANES)
                    spots = (t,) if t < half else (t, t + half)
                    if fold:
                        low = jnp.broadcast_to(cols[0, f, pl.ds(p, 1), at], (ROWS, LANES))
                        top = jnp.broadcast_to(cols[1, f, pl.ds(p, 1), at], (ROWS, LANES))
                        for n in spots:
                            full[n] = full[n] + added[0][n] * low
                            full[n] = full[n] + added[1][n] * top
                    e = full[t]
                    o = full[t + half] if t >= half else jnp.zeros((ROWS, LANES), F32)
                    out[k, f, p, 0, :, at] = jnp.where(is_even, e, pltpu.roll(o, 1, 0))
                    out[k, f, p, 1, :, at] = jnp.where(is_even, pltpu.roll(e, ROWS - 1, 0), o)
        put(k).start()

    def plain(k, _):
        one(k, False)
        return 0

    def folded(k, _):
        one(k, True)
        return 0

    lax.fori_loop(0, far, plain, 0)
    lax.fori_loop(far, groups, folded, 0)
    for k in range(groups):
        put(k).wait()


def in_hbm(x):
    return pltpu.with_memory_space_constraint(x, pltpu.HBM)


def body(forcing, slot_wavenumber, inverse, edge_weights):
    fields, points, halves, slots, degrees = forcing.shape
    subs, groups = lax.axis_size("sub"), lax.axis_size("ma")
    group = points // groups
    tiles = degrees // LANES
    half = tiles // 2
    wide = tiles + half
    assert halves == 2 and slots == ROWS and tiles == 4 and fields == 2
    assert groups >= 8 and groups & (groups - 1) == 0 and fields * group < MARK
    count = fields * group * tiles + 1
    end_count = tiles + 2
    value_count = fields * 2 * tiles + 1
    shape = jax.ShapeDtypeStruct
    blocks = points // ROWS
    dma = pltpu.SemaphoreType.DMA
    landed, values, cols = pl.pallas_call(
        functools.partial(solve_kernel, (fields, points, degrees, group, subs, groups)),
        in_specs=[pl.BlockSpec(memory_space=pltpu.HBM)] * 4,
        out_specs=[pl.BlockSpec(memory_space=pltpu.VMEM)] * 3,
        out_shape=[
            shape((groups, count, ROWS, LANES), F32),
            shape((2, value_count, ROWS, LANES), F32),
            shape((2, fields, group, degrees), F32),
        ],
        scratch_shapes=[
            pltpu.SMEM(slot_wavenumber.shape, slot_wavenumber.dtype),
            pltpu.SMEM(edge_weights.shape, F32),
            pltpu.VMEM((fields, points, halves, slots, degrees), F32),
            pltpu.VMEM((groups, fields, group, blocks, ROWS, degrees), F32),
            pltpu.VMEM((fields, points, tiles, ROWS, LANES), F32),
            pltpu.VMEM((fields, points, half, ROWS, LANES), F32),
            pltpu.VMEM((group, wide, ROWS, LANES), F32),
            pltpu.VMEM((groups - 4, group, wide, ROWS, LANES), F32),
            pltpu.VMEM((fields, blocks, 2, tiles, ROWS, LANES), F32),
            pltpu.VMEM((groups, count, ROWS, LANES), F32),
            pltpu.VMEM((groups, ROWS, LANES), F32),
            pltpu.VMEM((fields, 2, end_count, ROWS, LANES), F32),
            pltpu.VMEM((subs, fields, 2, end_count, ROWS, LANES), F32),
            pltpu.VMEM((fields, 2, wide, ROWS, LANES), F32),
            pltpu.VMEM((value_count, ROWS, LANES), F32),
            dma((2,)),
            dma((fields, 2)),
            dma((7,)),
            dma((2, fields)),
            dma((subs - 1, fields)),
            dma((subs - 1, fields)),
            dma((2,)),
            dma((2, fields)),
            dma((2, fields)),
        ],
        compiler_params=pltpu.CompilerParams(
            collective_id=0, has_side_effects=True, vmem_limit_bytes=VMEM_BYTES
        ),
    )(
        in_hbm(slot_wavenumber),
        in_hbm(edge_weights),
        in_hbm(forcing),
        in_hbm(inverse.reshape(1, fields, points, blocks, ROWS, degrees)),
    )

    return pl.pallas_call(
        functools.partial(finish_kernel, (fields, degrees, group, groups)),
        in_specs=[
            pl.BlockSpec(memory_space=pltpu.VMEM),
            pl.BlockSpec(memory_space=pltpu.VMEM),
            pl.BlockSpec(memory_space=pltpu.VMEM),
        ],
        out_specs=pl.BlockSpec(memory_space=pl.ANY),
        out_shape=shape((fields, group, halves, slots * groups, degrees), F32),
        scratch_shapes=[
            pltpu.VMEM((groups, fields, group, halves, slots, degrees), F32),
            dma((groups,)),
        ],
        compiler_params=pltpu.CompilerParams(vmem_limit_bytes=16 * 1024 * 1024),
    )(landed, values, cols)


def solution(mesh):
    return jax.shard_map(
        body,
        mesh=mesh,
        in_specs=(
            P(None, "sub", None, "ma", None),
            P("ma"),
            P("sub", None, None, None, None),
            P("sub", None, None),
        ),
        out_specs=P(None, ("sub", "ma"), None, None, None),
        check_vma=False,
    )
```

```python
import functools

import jax
import jax.numpy as jnp
from jax import lax
from jax.experimental import pallas as pl
from jax.experimental.pallas import tpu as pltpu
from jax.sharding import PartitionSpec as P

LANES = 128
ROWS = 8
F32 = jnp.float32
MESH = pl.DeviceIdType.MESH
MARK = 64
VMEM_BYTES = 40 * 1024 * 1024


def grid_iotas():
    row = lax.broadcasted_iota(jnp.int32, (ROWS, LANES), 0)
    lane = lax.broadcasted_iota(jnp.int32, (ROWS, LANES), 1)
    return row, lane


def lane_gather(values, index):
    return jnp.take_along_axis(values, index, axis=1, mode="promise_in_bounds")


def spread(values, k):
    return lane_gather(values, jnp.full((ROWS, LANES), k, jnp.int32))


def exclusive_or(a, b, groups):
    total = 0
    bit = 1
    while bit < groups:
        total = total + lax.rem(a // bit + b // bit, 2) * bit
        bit *= 2
    return total


def pack(pieces, m, degrees):
    _, lane = grid_iotas()
    shift_index = (lane - m) & (LANES - 1)
    left_index = (degrees - 1 - m) & (LANES - 1)
    near, far = pieces[4], pieces[5]
    near_moved = lane_gather(near, shift_index)
    far_moved = lane_gather(far, shift_index)
    first = jnp.where(
        lane >= m, pieces[0], jnp.where(lane - m >= -LANES, far_moved, near_moved)
    )
    second = jnp.where(lane + LANES >= m, pieces[1], far_moved)
    spare = jnp.where(m < LANES, lane_gather(far, left_index), lane_gather(near, left_index))
    return [first, second, pieces[2], pieces[3]], spare


def unpack(pieces, spare, m, degrees):
    _, lane = grid_iotas()
    back_index = (lane + m) & (LANES - 1)
    first = lane_gather(pieces[0], back_index)
    second = lane_gather(pieces[1], back_index)
    moved = [first, jnp.where(lane + m < 2 * LANES, first, second)]
    odd = []
    for t in range(2):
        degree = lane + (2 + t) * LANES
        odd.append(
            jnp.where(
                degree >= degrees - m,
                moved[t],
                jnp.where(degree == degrees - 1 - m, spare, 0.0),
            )
        )
    even = [
        jnp.where(lane >= m, pieces[0], 0.0),
        jnp.where(lane + LANES >= m, pieces[1], 0.0),
        pieces[2],
        pieces[3],
    ]
    return even + odd


def solve_kernel(
    dims, slot_in, edge_in, forcing, inverse, landed, values_landed, cols,
    slot, edge, raw, blocks_in, even_src, odd_src, part, stash, weighed, packed, lefts, ends,
    everyone, uvals, values,
    small_sem, raw_sem, in_sem, w_sem, z_send, z_recv, p_sem, u_sem, f_sem,
    ready,
):
    fields, points, degrees, group, subs, groups = dims
    tiles = degrees // LANES
    half = tiles // 2
    wide = tiles + half
    blocks = points // ROWS
    sub = lax.axis_index("sub")
    me = lax.axis_index("ma")
    row, lane = grid_iotas()
    is_even = (row & 1) == 0
    parity = lax.rem(me, 2)
    pair = me + 1 - 2 * parity
    far = groups - 2
    middle = groups - 4
    size = group * tiles
    mine = blocks // 2
    own_blocks = pl.ds(parity * mine, mine)
    its_blocks = pl.ds((1 - parity) * mine, mine)
    spot_left, spot_influence = tiles, tiles + 1

    def other(k):
        return exclusive_or(me, k, groups)

    def late_mask(j):
        return 2 + (middle // 2) * (1 - lax.rem(j, 2)) + j // 2

    def fetch(k, f, which, n):
        return pltpu.make_async_copy(
            inverse.at[0, f, pl.ds(other(k) * group, group), which],
            blocks_in.at[k, f, :, which],
            in_sem.at[n],
        )

    def arrived(count, f, which, n):
        target = blocks_in.at[pl.ds(0, count), f, :, which]
        pltpu.make_async_copy(target, target, in_sem.at[n]).wait()

    everything = pl.ds(0, blocks)

    def load(f, h):
        part_q = pl.ds(h * (points // 2), points // 2)
        return pltpu.make_async_copy(forcing.at[f, part_q], raw.at[f, part_q], raw_sem.at[f, h])

    def send(k, f, begin=0, end=None):
        if end is None:
            end = size + (f == fields - 1)
        rows = pl.ds(f * size + begin, end - begin)
        return pltpu.make_async_remote_copy(
            src_ref=packed.at[k, rows], dst_ref=landed.at[k, rows],
            send_sem=p_sem.at[0], recv_sem=p_sem.at[1],
            device_id=(sub, other(k)), device_id_type=MESH,
        )

    def value_rows(f):
        return pl.ds(f * 2 * tiles, 2 * tiles + (f == fields - 1))

    def send_values(f):
        return pltpu.make_async_remote_copy(
            src_ref=values.at[value_rows(f)], dst_ref=values_landed.at[0, value_rows(f)],
            send_sem=u_sem.at[0, f], recv_sem=u_sem.at[1, f],
            device_id=(sub, other(far)), device_id_type=MESH,
        )

    def forward(f):
        return pltpu.make_async_remote_copy(
            src_ref=values_landed.at[0, value_rows(f)], dst_ref=values_landed.at[1, value_rows(f)],
            send_sem=f_sem.at[0, f], recv_sem=f_sem.at[1, f],
            device_id=(sub, pair), device_id_type=MESH,
        )

    load(0, 0).start()
    load(0, 1).start()
    fetch(far + 1, 0, everything, 0).start()
    slot_copy = pltpu.make_async_copy(slot_in, slot, small_sem.at[0])
    edge_copy = pltpu.make_async_copy(edge_in, edge, small_sem.at[1])
    slot_copy.start()
    edge_copy.start()
    barrier = pltpu.get_barrier_semaphore()
    subs_to = [lax.rem(sub + n, subs) for n in range(1, subs)]
    for n in range(1, subs):
        @pl.when(sub + n < subs)
        def _(n=n):
            above = lax.rem(sub + n, subs)
            pl.semaphore_signal(barrier, inc=1, device_id=(above, me), device_id_type=MESH)
    for k in range(1, groups):
        pl.semaphore_signal(barrier, inc=1, device_id=(sub, other(k)), device_id_type=MESH)
    slot_copy.wait()
    edge_copy.wait()

    m = jnp.zeros((ROWS, LANES), jnp.int32)
    for j in range(ROWS // 2):
        m = jnp.where((row >> 1) == j, slot[2 * j], m)

    def prepare(f, h):
        def one(q):
            inside = jnp.where((q > 0) & (q < points - 1), 1.0, 0.0).astype(F32)
            for t in range(tiles):
                at = pl.ds(t * LANES, LANES)
                a = raw[f, q, 0, :, at] * inside
                b = raw[f, q, 1, :, at] * inside
                degree = lane + t * LANES
                mixed = jnp.where(is_even, a, pltpu.roll(b, 1, 0))
                even_src[f, q, t] = jnp.where(degree >= m, mixed, 0.0)
                if t >= half:
                    mixed = jnp.where(is_even, pltpu.roll(a, ROWS - 1, 0), b)
                    odd_src[f, q, t - half] = jnp.where(degree >= degrees - 1 - m, mixed, 0.0)

        def two(n, _):
            one(2 * n)
            one(2 * n + 1)
            return 0

        lax.fori_loop(h * (points // 4), (h + 1) * (points // 4), two, 0)

    def solve_half(k, f, into, begin=0, end=group):
        for span in (tuple(range(half)),) + tuple((t,) for t in range(half, tiles)):
            units = [(p, t, 0) for t in span for p in range(begin, end)]
            if span[0] >= half:
                units += [(p, t, 1) for t in span for p in range(begin, end)]

            def step(n, sums, span=span, units=units):
                sums = dict(zip(units, sums))
                for b in range(2):
                    block = 2 * n + b
                    for r in range(ROWS):
                        q = block * ROWS + r
                        for t in span:
                            even = even_src[f, q, t]
                            odd = odd_src[f, q, t - half] if t >= half else None
                            for p in range(begin, end):
                                line = blocks_in[
                                    k, f, p, block, pl.ds(r, 1), pl.ds(t * LANES, LANES)
                                ]
                                entry = jnp.broadcast_to(line, (ROWS, LANES))
                                sums[p, t, 0] += entry * even
                                if t >= half:
                                    sums[p, t, 1] += entry * odd
                return tuple(sums[unit] for unit in units)

            start = tuple(jnp.zeros((ROWS, LANES), F32) for _ in units)
            sums = lax.fori_loop(0, blocks // 2, step, start)
            for (p, t, o), total in zip(units, sums):
                into[p, t + half * o] = total

    def write_half(k, f, source, dest, fold, begin=0, end=group):
        if f == 0 and begin == 0:
            left = jnp.where(lane == MARK, m.astype(F32), 0.0)
        else:
            left = lefts[k]
        for p in range(begin, end):
            full = [source[p, t] for t in range(wide)]
            if fold:
                for t in range(tiles):
                    at = pl.ds(t * LANES, LANES)
                    line = blocks_in[k, f, p, 0, pl.ds(0, 1), at]
                    low = jnp.broadcast_to(line, (ROWS, LANES))
                    line = blocks_in[k, f, p, blocks - 1, pl.ds(ROWS - 1, 1), at]
                    top = jnp.broadcast_to(line, (ROWS, LANES))
                    for n in (t,) if t < half else (t, t + half):
                        full[n] = full[n] + uvals[f, 0, n] * low
                        full[n] = full[n] + uvals[f, 1, n] * top
            pieces, spare = pack(full, m, degrees)
            for t in range(tiles):
                dest[f * size + p * tiles + t] = pieces[t]
            left = jnp.where(lane == f * group + p, spare, left)
        if f == fields - 1 and end == group:
            dest[fields * size] = left
        else:
            lefts[k] = left

    def early(k, f):
        solve_half(k, f, part)
        write_half(k, f, part, packed.at[k], False)
        send(k, f).start()

    def weigh(f):
        def add(k, sums):
            sums = list(sums)
            for p in range(group):
                low = edge[0, 0, other(k) * group + p]
                top = edge[0, 1, other(k) * group + p]
                for b in range(mine):
                    for t in range(tiles):
                        at = parity * mine + b
                        entry = blocks_in[k, f, p, at, :, pl.ds(t * LANES, LANES)]
                        n = b * tiles + t
                        sums[n] += low * entry
                        sums[mine * tiles + n] += top * entry
            return tuple(sums)

        start = tuple(jnp.zeros((ROWS, LANES), F32) for _ in range(2 * mine * tiles))
        sums = lax.fori_loop(0, groups, add, start)
        for e in range(2):
            for b in range(mine):
                for t in range(tiles):
                    weighed[f, parity * mine + b, e, t] = sums[(e * mine + b) * tiles + t]

    def swap(f):
        shared = weighed.at[f, own_blocks]
        return pltpu.make_async_remote_copy(
            src_ref=shared, dst_ref=shared, send_sem=w_sem.at[0, f], recv_sem=w_sem.at[1, f],
            device_id=(sub, pair), device_id_type=MESH,
        )

    def exchange(n, f, sender, begin):
        outer = (sender == 0) | (sender == subs - 1)
        first = 1 - lax.min(sender, 1)
        for count, case in ((1, outer), (2, jnp.logical_not(outer))):
            kept = pl.ds(first, count) if count == 1 else pl.ds(0, 2)
            copy = pltpu.make_async_remote_copy(
                src_ref=ends.at[f, kept], dst_ref=everyone.at[sender, f, kept],
                send_sem=z_send.at[n, f], recv_sem=z_recv.at[n, f],
                device_id=(subs_to[n], me), device_id_type=MESH,
            )

            @pl.when(case)
            def _(copy=copy):
                begin(copy)

    def slopes(f):
        def slope_step(block, sums):
            sums = list(sums)
            for r in range(ROWS):
                q = block * ROWS + r
                for t in range(tiles):
                    even = even_src[f, q, t]
                    odd = odd_src[f, q, t - half] if t >= half else None
                    for e in range(2):
                        line = weighed[f, block, e, t, pl.ds(r, 1), :]
                        entry = jnp.broadcast_to(line, (ROWS, LANES))
                        sums[e * wide + t] += entry * even
                        if t >= half:
                            sums[e * wide + t + half] += entry * odd
            return tuple(sums)

        start = tuple(jnp.zeros((ROWS, LANES), F32) for _ in range(2 * wide))
        sums = lax.fori_loop(0, blocks, slope_step, start)
        for e in range(2):
            pieces, spare = pack(list(sums[e * wide:(e + 1) * wide]), m, degrees)
            for t in range(tiles):
                ends[f, e, t] = pieces[t]
            ends[f, e, spot_left] = spare
            for w in range(2):
                for t in range(tiles):
                    line = weighed[f, w * (blocks - 1), e, t, pl.ds(w * (ROWS - 1), 1), :]
                    ends[f, e, spot_influence, pl.ds(2 * t + w, 1), :] = line
        for n in range(subs - 1):
            exchange(n, f, sub, lambda copy: copy.start())
        everyone[sub, f] = ends[f]

    def interface(f):
        for n in range(subs - 1):
            exchange(n, f, sub, lambda copy: copy.wait_send())
            sender = lax.rem(sub + subs - n - 1, subs)
            exchange(n, f, sender, lambda copy: copy.wait_recv())

        def slopes_of(s, e):
            pieces = [everyone[s, f, e, t] for t in range(tiles)]
            return unpack(pieces, everyone[s, f, e, spot_left], m, degrees)

        rights = []
        for k in range(subs - 1):
            low, top = slopes_of(k + 1, 0), slopes_of(k, 1)
            rights.append([low[t] - top[t] for t in range(wide)])
        lower, upper = [], []
        for t in range(wide):
            source = t if t < tiles else t - half

            def influence(s, e, w):
                line = everyone[s, f, e, spot_influence, pl.ds(2 * source + w, 1), :]
                return jnp.broadcast_to(line, (ROWS, LANES))

            zero = jnp.zeros((ROWS, LANES), F32)
            ratio, reduced = zero, zero
            ratios, reduceds = [], []
            for k in range(subs - 1):
                low = influence(k, 1, 0)
                diagonal = influence(k, 1, 1) - influence(k + 1, 0, 0)
                up = -influence(k + 1, 0, 1)
                pivot = diagonal - low * ratio
                reduced = (rights[k][t] - low * reduced) / pivot
                ratio = up / pivot
                ratios.append(ratio)
                reduceds.append(reduced)
            later = zero
            lower_value, upper_value = zero, zero
            for k in range(subs - 2, -1, -1):
                later = reduceds[k] - ratios[k] * later
                lower_value = jnp.where(sub == k + 1, later, lower_value)
                upper_value = jnp.where(sub == k, later, upper_value)
            lower.append(lower_value)
            upper.append(upper_value)
        spares = values[fields * 2 * tiles] if f else jnp.zeros((ROWS, LANES), F32)
        for e, vector in enumerate((lower, upper)):
            for t in range(wide):
                uvals[f, e, t] = vector[t]
            pieces, spare = pack(vector, m, degrees)
            for t in range(tiles):
                values[f * 2 * tiles + e * tiles + t] = pieces[t]
            spares = jnp.where(lane == 2 * f + e, spare, spares)
        values[fields * 2 * tiles] = spares
        send_values(f).start()

    def late_parts(j, f):
        solve_half(late_mask(j), f, stash.at[j])

    def late_write(f):
        def one(j, _):
            k = late_mask(j)
            write_half(k, f, stash.at[j], packed.at[k], True)
            send(k, f).start()
            return 0

        lax.fori_loop(0, middle, one, 0)

    load(0, 0).wait()
    for k in range(far + 1):
        fetch(k, 0, own_blocks, 1).start()
    prepare(0, 0)
    load(0, 1).wait()
    fetch(far, 0, its_blocks, 2).start()
    prepare(0, 1)
    fetch(far + 1, 0, everything, 0).wait()
    for k in range(far):
        fetch(k, 0, its_blocks, 3).start()
    for h in range(2):
        load(1, h).start()
    quarter = group // 2
    solve_half(far + 1, 0, part, 0, quarter)
    write_half(far + 1, 0, part, packed.at[far + 1], False, 0, quarter)
    pl.semaphore_wait(barrier, groups - 1 + sub)
    send(far + 1, 0, 0, quarter * tiles).start()
    for n in range(1, subs):
        @pl.when(sub >= n)
        def _(n=n):
            below = lax.rem(sub + subs - n, subs)
            pl.semaphore_signal(ready, inc=1, device_id=(below, me), device_id_type=MESH)
    for k in (far + 1, far):
        fetch(k, 1, everything, 4 + far + 1 - k).start()
    solve_half(far + 1, 0, part, quarter, group)
    write_half(far + 1, 0, part, packed.at[far + 1], False, quarter, group)
    send(far + 1, 0, quarter * tiles).start()
    arrived(far + 1, 0, own_blocks, 1)
    for k in range(far):
        fetch(k, 1, everything, 6).start()
    weigh(0)
    swap(0).start()
    fetch(far, 0, its_blocks, 2).wait()
    early(far, 0)
    swap(0).wait()

    @pl.when(sub < subs - 1)
    def _():
        pl.semaphore_wait(ready, subs - 1 - sub)

    slopes(0)
    for h in range(2):
        load(1, h).wait()
        prepare(1, h)
    fetch(far + 1, 1, everything, 4).wait()
    early(far + 1, 1)
    fetch(far, 1, everything, 5).wait()
    early(far, 1)
    arrived(far, 0, its_blocks, 3)
    arrived(far, 1, everything, 6)
    weigh(1)
    swap(1).start()
    late_parts(0, 0)
    swap(1).wait()
    slopes(1)
    for f in range(fields):
        def more(j, _, f=f):
            late_parts(j, f)
            return 0

        lax.fori_loop(1 if f == 0 else 0, middle, more, 0)
        interface(f)
        late_write(f)

    for f in range(fields):
        solve_half(1, f, part)
        write_half(1, f, part, packed.at[1], True)
        send(1, f).start()
    for f in range(fields):
        send_values(f).wait_recv()
        forward(f).start()
    for f in range(fields):
        solve_half(0, f, part)
        write_half(0, f, part, landed.at[0], True)
    for f in range(fields):
        for p in range(group):
            cols[0, f, pl.ds(p, 1), :] = blocks_in[0, f, p, 0, pl.ds(0, 1), :]
            cols[1, f, pl.ds(p, 1), :] = blocks_in[0, f, p, blocks - 1, pl.ds(ROWS - 1, 1), :]
    for f in range(fields):
        send_values(f).wait_send()
        forward(f).wait()
    away = pl.ds(1, groups - 1)
    pltpu.make_async_remote_copy(
        src_ref=packed.at[away], dst_ref=landed.at[away],
        send_sem=p_sem.at[0], recv_sem=p_sem.at[1],
        device_id=(sub, pair), device_id_type=MESH,
    ).wait()


def finish_kernel(dims, landed, values, cols, result, out, out_sem):
    fields, degrees, group, groups = dims
    tiles = degrees // LANES
    half = tiles // 2
    me = lax.axis_index("ma")
    row, _ = grid_iotas()
    is_even = (row & 1) == 0
    far = groups - 2

    def put(k):
        at = exclusive_or(me, k, groups) * ROWS
        rows = pl.ds(pl.multiple_of(at, ROWS), ROWS)
        return pltpu.make_async_copy(out.at[k], result.at[:, :, :, rows, :], out_sem.at[k])

    def one(k, fold):
        left = landed[k, fields * group * tiles]
        m = spread(left, MARK).astype(jnp.int32)
        for f in range(fields):
            added = []
            for e in range(2 if fold else 0):
                at = (2 * f + e) * tiles
                pieces = [values[k - far, at + t] for t in range(tiles)]
                spare = spread(values[k - far, fields * 2 * tiles], 2 * f + e)
                added.append(unpack(pieces, spare, m, degrees))
            for p in range(group):
                n = f * group + p
                pieces = [landed[k, n * tiles + t] for t in range(tiles)]
                full = unpack(pieces, spread(left, n), m, degrees)
                for t in range(tiles):
                    at = pl.ds(t * LANES, LANES)
                    spots = (t,) if t < half else (t, t + half)
                    if fold:
                        low = jnp.broadcast_to(cols[0, f, pl.ds(p, 1), at], (ROWS, LANES))
                        top = jnp.broadcast_to(cols[1, f, pl.ds(p, 1), at], (ROWS, LANES))
                        for n in spots:
                            full[n] = full[n] + added[0][n] * low
                            full[n] = full[n] + added[1][n] * top
                    e = full[t]
                    o = full[t + half] if t >= half else jnp.zeros((ROWS, LANES), F32)
                    out[k, f, p, 0, :, at] = jnp.where(is_even, e, pltpu.roll(o, 1, 0))
                    out[k, f, p, 1, :, at] = jnp.where(is_even, pltpu.roll(e, ROWS - 1, 0), o)
        put(k).start()

    def plain(k, _):
        one(k, False)
        return 0

    def folded(k, _):
        one(k, True)
        return 0

    lax.fori_loop(0, far, plain, 0)
    lax.fori_loop(far, groups, folded, 0)
    for k in range(groups):
        put(k).wait()


def in_hbm(x):
    return pltpu.with_memory_space_constraint(x, pltpu.HBM)


def body(forcing, slot_wavenumber, inverse, edge_weights):
    fields, points, halves, slots, degrees = forcing.shape
    subs, groups = lax.axis_size("sub"), lax.axis_size("ma")
    group = points // groups
    tiles = degrees // LANES
    half = tiles // 2
    wide = tiles + half
    assert halves == 2 and slots == ROWS and tiles == 4 and fields == 2
    assert groups >= 8 and groups & (groups - 1) == 0 and fields * group < MARK
    count = fields * group * tiles + 1
    end_count = tiles + 2
    value_count = fields * 2 * tiles + 1
    shape = jax.ShapeDtypeStruct
    blocks = points // ROWS
    dma = pltpu.SemaphoreType.DMA
    landed, values, cols = pl.pallas_call(
        functools.partial(solve_kernel, (fields, points, degrees, group, subs, groups)),
        in_specs=[pl.BlockSpec(memory_space=pltpu.HBM)] * 4,
        out_specs=[pl.BlockSpec(memory_space=pltpu.VMEM)] * 3,
        out_shape=[
            shape((groups, count, ROWS, LANES), F32),
            shape((2, value_count, ROWS, LANES), F32),
            shape((2, fields, group, degrees), F32),
        ],
        scratch_shapes=[
            pltpu.SMEM(slot_wavenumber.shape, slot_wavenumber.dtype),
            pltpu.SMEM(edge_weights.shape, F32),
            pltpu.VMEM((fields, points, halves, slots, degrees), F32),
            pltpu.VMEM((groups, fields, group, blocks, ROWS, degrees), F32),
            pltpu.VMEM((fields, points, tiles, ROWS, LANES), F32),
            pltpu.VMEM((fields, points, half, ROWS, LANES), F32),
            pltpu.VMEM((group, wide, ROWS, LANES), F32),
            pltpu.VMEM((groups - 4, group, wide, ROWS, LANES), F32),
            pltpu.VMEM((fields, blocks, 2, tiles, ROWS, LANES), F32),
            pltpu.VMEM((groups, count, ROWS, LANES), F32),
            pltpu.VMEM((groups, ROWS, LANES), F32),
            pltpu.VMEM((fields, 2, end_count, ROWS, LANES), F32),
            pltpu.VMEM((subs, fields, 2, end_count, ROWS, LANES), F32),
            pltpu.VMEM((fields, 2, wide, ROWS, LANES), F32),
            pltpu.VMEM((value_count, ROWS, LANES), F32),
            dma((2,)),
            dma((fields, 2)),
            dma((7,)),
            dma((2, fields)),
            dma((subs - 1, fields)),
            dma((subs - 1, fields)),
            dma((2,)),
            dma((2, fields)),
            dma((2, fields)),
            pltpu.SemaphoreType.REGULAR,
        ],
        compiler_params=pltpu.CompilerParams(
            collective_id=0, has_side_effects=True, vmem_limit_bytes=VMEM_BYTES
        ),
    )(
        in_hbm(slot_wavenumber),
        in_hbm(edge_weights),
        in_hbm(forcing),
        in_hbm(inverse.reshape(1, fields, points, blocks, ROWS, degrees)),
    )

    return pl.pallas_call(
        functools.partial(finish_kernel, (fields, degrees, group, groups)),
        in_specs=[
            pl.BlockSpec(memory_space=pltpu.VMEM),
            pl.BlockSpec(memory_space=pltpu.VMEM),
            pl.BlockSpec(memory_space=pltpu.VMEM),
        ],
        out_specs=pl.BlockSpec(memory_space=pl.ANY),
        out_shape=shape((fields, group, halves, slots * groups, degrees), F32),
        scratch_shapes=[
            pltpu.VMEM((groups, fields, group, halves, slots, degrees), F32),
            dma((groups,)),
        ],
        compiler_params=pltpu.CompilerParams(vmem_limit_bytes=16 * 1024 * 1024),
    )(landed, values, cols)


def solution(mesh):
    return jax.shard_map(
        body,
        mesh=mesh,
        in_specs=(
            P(None, "sub", None, "ma", None),
            P("ma"),
            P("sub", None, None, None, None),
            P("sub", None, None),
        ),
        out_specs=P(None, ("sub", "ma"), None, None, None),
        check_vma=False,
    )
```

```python
import functools

import jax
import jax.numpy as jnp
from jax import lax
from jax.experimental import pallas as pl
from jax.experimental.pallas import tpu as pltpu
from jax.sharding import PartitionSpec as P

LANES = 128
ROWS = 8
F32 = jnp.float32
MESH = pl.DeviceIdType.MESH
MARK = 64
VMEM_BYTES = 40 * 1024 * 1024


def grid_iotas():
    row = lax.broadcasted_iota(jnp.int32, (ROWS, LANES), 0)
    lane = lax.broadcasted_iota(jnp.int32, (ROWS, LANES), 1)
    return row, lane


def lane_gather(values, index):
    return jnp.take_along_axis(values, index, axis=1, mode="promise_in_bounds")


def spread(values, k):
    return lane_gather(values, jnp.full((ROWS, LANES), k, jnp.int32))


def exclusive_or(a, b, groups):
    total = 0
    bit = 1
    while bit < groups:
        total = total + lax.rem(a // bit + b // bit, 2) * bit
        bit *= 2
    return total


def pack(pieces, m, degrees):
    _, lane = grid_iotas()
    shift_index = (lane - m) & (LANES - 1)
    left_index = (degrees - 1 - m) & (LANES - 1)
    near, far = pieces[4], pieces[5]
    near_moved = lane_gather(near, shift_index)
    far_moved = lane_gather(far, shift_index)
    first = jnp.where(
        lane >= m, pieces[0], jnp.where(lane - m >= -LANES, far_moved, near_moved)
    )
    second = jnp.where(lane + LANES >= m, pieces[1], far_moved)
    spare = jnp.where(m < LANES, lane_gather(far, left_index), lane_gather(near, left_index))
    return [first, second, pieces[2], pieces[3]], spare


def unpack(pieces, spare, m, degrees):
    _, lane = grid_iotas()
    back_index = (lane + m) & (LANES - 1)
    first = lane_gather(pieces[0], back_index)
    second = lane_gather(pieces[1], back_index)
    moved = [first, jnp.where(lane + m < 2 * LANES, first, second)]
    odd = []
    for t in range(2):
        degree = lane + (2 + t) * LANES
        odd.append(
            jnp.where(
                degree >= degrees - m,
                moved[t],
                jnp.where(degree == degrees - 1 - m, spare, 0.0),
            )
        )
    even = [
        jnp.where(lane >= m, pieces[0], 0.0),
        jnp.where(lane + LANES >= m, pieces[1], 0.0),
        pieces[2],
        pieces[3],
    ]
    return even + odd


def value_row(f, e, fields, tiles):
    return (2 * f + e) * tiles + (e if f == fields - 1 else 0)


def spare_row(fields, tiles):
    return (2 * fields - 1) * tiles


def solve_kernel(
    dims, slot_in, edge_in, forcing, inverse, landed, values_landed, cols,
    slot, edge, raw, blocks_in, even_src, odd_src, part, stash, weighed, packed, lefts, ends,
    everyone, uvals, values,
    small_sem, raw_sem, in_sem, w_sem, z_send, z_recv, p_sem, u_sem, f_sem,
    ready,
):
    fields, points, degrees, group, subs, groups = dims
    tiles = degrees // LANES
    half = tiles // 2
    wide = tiles + half
    blocks = points // ROWS
    sub = lax.axis_index("sub")
    me = lax.axis_index("ma")
    row, lane = grid_iotas()
    is_even = (row & 1) == 0
    parity = lax.rem(me, 2)
    pair = me + 1 - 2 * parity
    far = groups - 2
    middle = groups - 4
    size = group * tiles
    mine = blocks // 2
    own_blocks = pl.ds(parity * mine, mine)
    its_blocks = pl.ds((1 - parity) * mine, mine)
    spot_left, spot_influence = tiles, tiles + 1

    def other(k):
        return exclusive_or(me, k, groups)

    def late_mask(j):
        return 2 + (middle // 2) * (1 - lax.rem(j, 2)) + j // 2

    def fetch(k, f, which, n):
        return pltpu.make_async_copy(
            inverse.at[0, f, pl.ds(other(k) * group, group), which],
            blocks_in.at[k, f, :, which],
            in_sem.at[n],
        )

    def arrived(count, f, which, n):
        target = blocks_in.at[pl.ds(0, count), f, :, which]
        pltpu.make_async_copy(target, target, in_sem.at[n]).wait()

    everything = pl.ds(0, blocks)

    def load(f, h):
        part_q = pl.ds(h * (points // 2), points // 2)
        return pltpu.make_async_copy(forcing.at[f, part_q], raw.at[f, part_q], raw_sem.at[f, h])

    def send(k, f, begin=0, end=None):
        if end is None:
            end = size + (f == fields - 1)
        rows = pl.ds(f * size + begin, end - begin)
        return pltpu.make_async_remote_copy(
            src_ref=packed.at[k, rows], dst_ref=landed.at[k, rows],
            send_sem=p_sem.at[0], recv_sem=p_sem.at[1],
            device_id=(sub, other(k)), device_id_type=MESH,
        )

    def send_values(f, begin):
        two_sided(f, begin, values, values_landed.at[0], u_sem, other(far))

    def forward(f, begin):
        two_sided(f, begin, values_landed.at[0], values_landed.at[1], f_sem, pair)

    def two_sided(f, begin, source, dest, sem, to):
        outer = (sub == 0) | (sub == subs - 1)
        more = f == fields - 1
        skip = (1 - lax.min(sub, 1)) * tiles
        inner_rows = pl.ds(f * 2 * tiles, 2 * tiles + more)
        outer_rows = pl.ds(f * 2 * tiles + skip, tiles + more)
        for case, rows in ((outer, outer_rows), (jnp.logical_not(outer), inner_rows)):
            copy = pltpu.make_async_remote_copy(
                src_ref=source.at[rows], dst_ref=dest.at[rows],
                send_sem=sem.at[0, f], recv_sem=sem.at[1, f],
                device_id=(sub, to), device_id_type=MESH,
            )

            @pl.when(case)
            def _(copy=copy):
                begin(copy)

    def clear(e):
        for f in range(fields):
            for slot_of in range(2):
                for t in range(tiles):
                    at = value_row(f, e, fields, tiles) + t
                    values_landed[slot_of, at] = jnp.zeros((ROWS, LANES), F32)

    load(0, 0).start()
    load(0, 1).start()
    fetch(far + 1, 0, everything, 0).start()
    slot_copy = pltpu.make_async_copy(slot_in, slot, small_sem.at[0])
    edge_copy = pltpu.make_async_copy(edge_in, edge, small_sem.at[1])
    slot_copy.start()
    edge_copy.start()
    barrier = pltpu.get_barrier_semaphore()

    @pl.when(sub == 0)
    def _():
        clear(0)

    @pl.when(sub == subs - 1)
    def _():
        clear(1)

    subs_to = [lax.rem(sub + n, subs) for n in range(1, subs)]
    for n in range(1, subs):
        @pl.when(sub + n < subs)
        def _(n=n):
            above = lax.rem(sub + n, subs)
            pl.semaphore_signal(barrier, inc=1, device_id=(above, me), device_id_type=MESH)
    for k in range(1, groups):
        pl.semaphore_signal(barrier, inc=1, device_id=(sub, other(k)), device_id_type=MESH)
    slot_copy.wait()
    edge_copy.wait()

    m = jnp.zeros((ROWS, LANES), jnp.int32)
    for j in range(ROWS // 2):
        m = jnp.where((row >> 1) == j, slot[2 * j], m)

    def prepare(f, h):
        def one(q):
            inside = jnp.where((q > 0) & (q < points - 1), 1.0, 0.0).astype(F32)
            for t in range(tiles):
                at = pl.ds(t * LANES, LANES)
                a = raw[f, q, 0, :, at] * inside
                b = raw[f, q, 1, :, at] * inside
                degree = lane + t * LANES
                mixed = jnp.where(is_even, a, pltpu.roll(b, 1, 0))
                even_src[f, q, t] = jnp.where(degree >= m, mixed, 0.0)
                if t >= half:
                    mixed = jnp.where(is_even, pltpu.roll(a, ROWS - 1, 0), b)
                    odd_src[f, q, t - half] = jnp.where(degree >= degrees - 1 - m, mixed, 0.0)

        def two(n, _):
            one(2 * n)
            one(2 * n + 1)
            return 0

        lax.fori_loop(h * (points // 4), (h + 1) * (points // 4), two, 0)

    def solve_half(k, f, into, begin=0, end=group):
        for span in (tuple(range(half)),) + tuple((t,) for t in range(half, tiles)):
            units = [(p, t, 0) for t in span for p in range(begin, end)]
            if span[0] >= half:
                units += [(p, t, 1) for t in span for p in range(begin, end)]

            def step(n, sums, span=span, units=units):
                sums = dict(zip(units, sums))
                for b in range(2):
                    block = 2 * n + b
                    for r in range(ROWS):
                        q = block * ROWS + r
                        for t in span:
                            even = even_src[f, q, t]
                            odd = odd_src[f, q, t - half] if t >= half else None
                            for p in range(begin, end):
                                line = blocks_in[
                                    k, f, p, block, pl.ds(r, 1), pl.ds(t * LANES, LANES)
                                ]
                                entry = jnp.broadcast_to(line, (ROWS, LANES))
                                sums[p, t, 0] += entry * even
                                if t >= half:
                                    sums[p, t, 1] += entry * odd
                return tuple(sums[unit] for unit in units)

            start = tuple(jnp.zeros((ROWS, LANES), F32) for _ in units)
            sums = lax.fori_loop(0, blocks // 2, step, start)
            for (p, t, o), total in zip(units, sums):
                into[p, t + half * o] = total

    def write_half(k, f, source, dest, fold, begin=0, end=group):
        if f == 0 and begin == 0:
            left = jnp.where(lane == MARK, m.astype(F32), 0.0)
        else:
            left = lefts[k]
        for p in range(begin, end):
            full = [source[p, t] for t in range(wide)]
            if fold:
                for t in range(tiles):
                    at = pl.ds(t * LANES, LANES)
                    line = blocks_in[k, f, p, 0, pl.ds(0, 1), at]
                    low = jnp.broadcast_to(line, (ROWS, LANES))
                    line = blocks_in[k, f, p, blocks - 1, pl.ds(ROWS - 1, 1), at]
                    top = jnp.broadcast_to(line, (ROWS, LANES))
                    for n in (t,) if t < half else (t, t + half):
                        full[n] = full[n] + uvals[f, 0, n] * low
                        full[n] = full[n] + uvals[f, 1, n] * top
            pieces, spare = pack(full, m, degrees)
            for t in range(tiles):
                dest[f * size + p * tiles + t] = pieces[t]
            left = jnp.where(lane == f * group + p, spare, left)
        if f == fields - 1 and end == group:
            dest[fields * size] = left
        else:
            lefts[k] = left

    def early(k, f):
        solve_half(k, f, part)
        write_half(k, f, part, packed.at[k], False)
        send(k, f).start()

    def weigh(f):
        def add(k, sums):
            sums = list(sums)
            for p in range(group):
                low = edge[0, 0, other(k) * group + p]
                top = edge[0, 1, other(k) * group + p]
                for b in range(mine):
                    for t in range(tiles):
                        at = parity * mine + b
                        entry = blocks_in[k, f, p, at, :, pl.ds(t * LANES, LANES)]
                        n = b * tiles + t
                        sums[n] += low * entry
                        sums[mine * tiles + n] += top * entry
            return tuple(sums)

        start = tuple(jnp.zeros((ROWS, LANES), F32) for _ in range(2 * mine * tiles))
        sums = lax.fori_loop(0, groups, add, start)
        for e in range(2):
            for b in range(mine):
                for t in range(tiles):
                    weighed[f, parity * mine + b, e, t] = sums[(e * mine + b) * tiles + t]

    def swap(f):
        shared = weighed.at[f, own_blocks]
        return pltpu.make_async_remote_copy(
            src_ref=shared, dst_ref=shared, send_sem=w_sem.at[0, f], recv_sem=w_sem.at[1, f],
            device_id=(sub, pair), device_id_type=MESH,
        )

    def exchange(n, f, sender, begin):
        outer = (sender == 0) | (sender == subs - 1)
        first = 1 - lax.min(sender, 1)
        for count, case in ((1, outer), (2, jnp.logical_not(outer))):
            kept = pl.ds(first, count) if count == 1 else pl.ds(0, 2)
            copy = pltpu.make_async_remote_copy(
                src_ref=ends.at[f, kept], dst_ref=everyone.at[sender, f, kept],
                send_sem=z_send.at[n, f], recv_sem=z_recv.at[n, f],
                device_id=(subs_to[n], me), device_id_type=MESH,
            )

            @pl.when(case)
            def _(copy=copy):
                begin(copy)

    def slopes(f):
        def slope_step(block, sums):
            sums = list(sums)
            for r in range(ROWS):
                q = block * ROWS + r
                for t in range(tiles):
                    even = even_src[f, q, t]
                    odd = odd_src[f, q, t - half] if t >= half else None
                    for e in range(2):
                        line = weighed[f, block, e, t, pl.ds(r, 1), :]
                        entry = jnp.broadcast_to(line, (ROWS, LANES))
                        sums[e * wide + t] += entry * even
                        if t >= half:
                            sums[e * wide + t + half] += entry * odd
            return tuple(sums)

        start = tuple(jnp.zeros((ROWS, LANES), F32) for _ in range(2 * wide))
        sums = lax.fori_loop(0, blocks, slope_step, start)
        for e in range(2):
            pieces, spare = pack(list(sums[e * wide:(e + 1) * wide]), m, degrees)
            for t in range(tiles):
                ends[f, e, t] = pieces[t]
            ends[f, e, spot_left] = spare
            for w in range(2):
                for t in range(tiles):
                    line = weighed[f, w * (blocks - 1), e, t, pl.ds(w * (ROWS - 1), 1), :]
                    ends[f, e, spot_influence, pl.ds(2 * t + w, 1), :] = line
        for n in range(subs - 1):
            exchange(n, f, sub, lambda copy: copy.start())
        everyone[sub, f] = ends[f]

    def interface(f):
        for n in range(subs - 1):
            exchange(n, f, sub, lambda copy: copy.wait_send())
            sender = lax.rem(sub + subs - n - 1, subs)
            exchange(n, f, sender, lambda copy: copy.wait_recv())

        def slopes_of(s, e):
            pieces = [everyone[s, f, e, t] for t in range(tiles)]
            return unpack(pieces, everyone[s, f, e, spot_left], m, degrees)

        rights = []
        for k in range(subs - 1):
            low, top = slopes_of(k + 1, 0), slopes_of(k, 1)
            rights.append([low[t] - top[t] for t in range(wide)])
        lower, upper = [], []
        for t in range(wide):
            source = t if t < tiles else t - half

            def influence(s, e, w):
                line = everyone[s, f, e, spot_influence, pl.ds(2 * source + w, 1), :]
                return jnp.broadcast_to(line, (ROWS, LANES))

            zero = jnp.zeros((ROWS, LANES), F32)
            ratio, reduced = zero, zero
            ratios, reduceds = [], []
            for k in range(subs - 1):
                low = influence(k, 1, 0)
                diagonal = influence(k, 1, 1) - influence(k + 1, 0, 0)
                up = -influence(k + 1, 0, 1)
                pivot = diagonal - low * ratio
                reduced = (rights[k][t] - low * reduced) / pivot
                ratio = up / pivot
                ratios.append(ratio)
                reduceds.append(reduced)
            later = zero
            lower_value, upper_value = zero, zero
            for k in range(subs - 2, -1, -1):
                later = reduceds[k] - ratios[k] * later
                lower_value = jnp.where(sub == k + 1, later, lower_value)
                upper_value = jnp.where(sub == k, later, upper_value)
            lower.append(lower_value)
            upper.append(upper_value)
        spares = values[spare_row(fields, tiles)] if f else jnp.zeros((ROWS, LANES), F32)
        for e, vector in enumerate((lower, upper)):
            for t in range(wide):
                uvals[f, e, t] = vector[t]
            pieces, spare = pack(vector, m, degrees)
            for t in range(tiles):
                values[value_row(f, e, fields, tiles) + t] = pieces[t]
            spares = jnp.where(lane == 2 * f + e, spare, spares)
        values[spare_row(fields, tiles)] = spares
        send_values(f, lambda copy: copy.start())

    def late_parts(j, f):
        solve_half(late_mask(j), f, stash.at[j])

    def late_write(f, count):
        def one(j, _):
            k = late_mask(j)
            write_half(k, f, stash.at[j], packed.at[k], True)
            send(k, f).start()
            return 0

        lax.fori_loop(0, count, one, 0)

    load(0, 0).wait()
    for k in range(far + 1):
        fetch(k, 0, own_blocks, 1).start()
    prepare(0, 0)
    load(0, 1).wait()
    fetch(far, 0, its_blocks, 2).start()
    prepare(0, 1)
    fetch(far + 1, 0, everything, 0).wait()
    for k in range(far):
        fetch(k, 0, its_blocks, 3).start()
    for h in range(2):
        load(1, h).start()
    quarter = group // 2
    solve_half(far + 1, 0, part, 0, quarter)
    write_half(far + 1, 0, part, packed.at[far + 1], False, 0, quarter)
    pl.semaphore_wait(barrier, groups - 1 + sub)
    send(far + 1, 0, 0, quarter * tiles).start()
    for n in range(1, subs):
        @pl.when(sub >= n)
        def _(n=n):
            below = lax.rem(sub + subs - n, subs)
            pl.semaphore_signal(ready, inc=1, device_id=(below, me), device_id_type=MESH)
    for k in (far + 1, far):
        fetch(k, 1, everything, 4 + far + 1 - k).start()
    solve_half(far + 1, 0, part, quarter, group)
    write_half(far + 1, 0, part, packed.at[far + 1], False, quarter, group)
    send(far + 1, 0, quarter * tiles).start()
    arrived(far + 1, 0, own_blocks, 1)
    for k in range(far):
        fetch(k, 1, everything, 6).start()
    weigh(0)
    swap(0).start()
    fetch(far, 0, its_blocks, 2).wait()
    early(far, 0)
    swap(0).wait()

    @pl.when(sub < subs - 1)
    def _():
        pl.semaphore_wait(ready, subs - 1 - sub)

    slopes(0)
    for h in range(2):
        load(1, h).wait()
        prepare(1, h)
    fetch(far + 1, 1, everything, 4).wait()
    early(far + 1, 1)
    fetch(far, 1, everything, 5).wait()
    early(far, 1)
    arrived(far, 0, its_blocks, 3)
    arrived(far, 1, everything, 6)
    weigh(1)
    swap(1).start()
    late_parts(0, 0)
    swap(1).wait()
    slopes(1)
    for f in range(fields):
        def more(j, _, f=f):
            late_parts(j, f)
            return 0

        begin, end = (1, middle) if f == 0 else (0, middle - 1)
        lax.fori_loop(begin, end, more, 0)
        interface(f)
        late_write(f, end)
        for j in range(end, middle):
            k = late_mask(j)
            solve_half(k, f, part)
            write_half(k, f, part, packed.at[k], True)
            send(k, f).start()

    for f in range(fields):
        solve_half(1, f, part)
        write_half(1, f, part, packed.at[1], True)
        send(1, f).start()
    for f in range(fields):
        send_values(f, lambda copy: copy.wait_recv())
        forward(f, lambda copy: copy.start())
    for f in range(fields):
        solve_half(0, f, part)
        write_half(0, f, part, landed.at[0], True)
    for f in range(fields):
        for p in range(group):
            cols[0, f, pl.ds(p, 1), :] = blocks_in[0, f, p, 0, pl.ds(0, 1), :]
            cols[1, f, pl.ds(p, 1), :] = blocks_in[0, f, p, blocks - 1, pl.ds(ROWS - 1, 1), :]
    for f in range(fields):
        send_values(f, lambda copy: copy.wait_send())
        forward(f, lambda copy: copy.wait())
    away = pl.ds(1, groups - 1)
    pltpu.make_async_remote_copy(
        src_ref=packed.at[away], dst_ref=landed.at[away],
        send_sem=p_sem.at[0], recv_sem=p_sem.at[1],
        device_id=(sub, pair), device_id_type=MESH,
    ).wait()


def finish_kernel(dims, landed, values, cols, result, out, out_sem):
    fields, degrees, group, groups = dims
    tiles = degrees // LANES
    half = tiles // 2
    me = lax.axis_index("ma")
    row, _ = grid_iotas()
    is_even = (row & 1) == 0
    far = groups - 2

    def put(k):
        at = exclusive_or(me, k, groups) * ROWS
        rows = pl.ds(pl.multiple_of(at, ROWS), ROWS)
        return pltpu.make_async_copy(out.at[k], result.at[:, :, :, rows, :], out_sem.at[k])

    def one(k, fold):
        left = landed[k, fields * group * tiles]
        m = spread(left, MARK).astype(jnp.int32)
        for f in range(fields):
            added = []
            for e in range(2 if fold else 0):
                at = value_row(f, e, fields, tiles)
                pieces = [values[k - far, at + t] for t in range(tiles)]
                spare = spread(values[k - far, spare_row(fields, tiles)], 2 * f + e)
                added.append(unpack(pieces, spare, m, degrees))
            for p in range(group):
                n = f * group + p
                pieces = [landed[k, n * tiles + t] for t in range(tiles)]
                full = unpack(pieces, spread(left, n), m, degrees)
                for t in range(tiles):
                    at = pl.ds(t * LANES, LANES)
                    spots = (t,) if t < half else (t, t + half)
                    if fold:
                        low = jnp.broadcast_to(cols[0, f, pl.ds(p, 1), at], (ROWS, LANES))
                        top = jnp.broadcast_to(cols[1, f, pl.ds(p, 1), at], (ROWS, LANES))
                        for n in spots:
                            full[n] = full[n] + added[0][n] * low
                            full[n] = full[n] + added[1][n] * top
                    e = full[t]
                    o = full[t + half] if t >= half else jnp.zeros((ROWS, LANES), F32)
                    out[k, f, p, 0, :, at] = jnp.where(is_even, e, pltpu.roll(o, 1, 0))
                    out[k, f, p, 1, :, at] = jnp.where(is_even, pltpu.roll(e, ROWS - 1, 0), o)
        put(k).start()

    def plain(k, _):
        one(k, False)
        return 0

    def folded(k, _):
        one(k, True)
        return 0

    lax.fori_loop(0, far, plain, 0)
    lax.fori_loop(far, groups, folded, 0)
    for k in range(groups):
        put(k).wait()


def in_hbm(x):
    return pltpu.with_memory_space_constraint(x, pltpu.HBM)


def body(forcing, slot_wavenumber, inverse, edge_weights):
    fields, points, halves, slots, degrees = forcing.shape
    subs, groups = lax.axis_size("sub"), lax.axis_size("ma")
    group = points // groups
    tiles = degrees // LANES
    half = tiles // 2
    wide = tiles + half
    assert halves == 2 and slots == ROWS and tiles == 4 and fields == 2
    assert groups >= 8 and groups & (groups - 1) == 0 and fields * group < MARK
    count = fields * group * tiles + 1
    end_count = tiles + 2
    value_count = fields * 2 * tiles + 1
    shape = jax.ShapeDtypeStruct
    blocks = points // ROWS
    dma = pltpu.SemaphoreType.DMA
    landed, values, cols = pl.pallas_call(
        functools.partial(solve_kernel, (fields, points, degrees, group, subs, groups)),
        in_specs=[pl.BlockSpec(memory_space=pltpu.HBM)] * 4,
        out_specs=[pl.BlockSpec(memory_space=pltpu.VMEM)] * 3,
        out_shape=[
            shape((groups, count, ROWS, LANES), F32),
            shape((2, value_count, ROWS, LANES), F32),
            shape((2, fields, group, degrees), F32),
        ],
        scratch_shapes=[
            pltpu.SMEM(slot_wavenumber.shape, slot_wavenumber.dtype),
            pltpu.SMEM(edge_weights.shape, F32),
            pltpu.VMEM((fields, points, halves, slots, degrees), F32),
            pltpu.VMEM((groups, fields, group, blocks, ROWS, degrees), F32),
            pltpu.VMEM((fields, points, tiles, ROWS, LANES), F32),
            pltpu.VMEM((fields, points, half, ROWS, LANES), F32),
            pltpu.VMEM((group, wide, ROWS, LANES), F32),
            pltpu.VMEM((groups - 4, group, wide, ROWS, LANES), F32),
            pltpu.VMEM((fields, blocks, 2, tiles, ROWS, LANES), F32),
            pltpu.VMEM((groups, count, ROWS, LANES), F32),
            pltpu.VMEM((groups, ROWS, LANES), F32),
            pltpu.VMEM((fields, 2, end_count, ROWS, LANES), F32),
            pltpu.VMEM((subs, fields, 2, end_count, ROWS, LANES), F32),
            pltpu.VMEM((fields, 2, wide, ROWS, LANES), F32),
            pltpu.VMEM((value_count, ROWS, LANES), F32),
            dma((2,)),
            dma((fields, 2)),
            dma((7,)),
            dma((2, fields)),
            dma((subs - 1, fields)),
            dma((subs - 1, fields)),
            dma((2,)),
            dma((2, fields)),
            dma((2, fields)),
            pltpu.SemaphoreType.REGULAR,
        ],
        compiler_params=pltpu.CompilerParams(
            collective_id=0, has_side_effects=True, vmem_limit_bytes=VMEM_BYTES
        ),
    )(
        in_hbm(slot_wavenumber),
        in_hbm(edge_weights),
        in_hbm(forcing),
        in_hbm(inverse.reshape(1, fields, points, blocks, ROWS, degrees)),
    )

    return pl.pallas_call(
        functools.partial(finish_kernel, (fields, degrees, group, groups)),
        in_specs=[
            pl.BlockSpec(memory_space=pltpu.VMEM),
            pl.BlockSpec(memory_space=pltpu.VMEM),
            pl.BlockSpec(memory_space=pltpu.VMEM),
        ],
        out_specs=pl.BlockSpec(memory_space=pl.ANY),
        out_shape=shape((fields, group, halves, slots * groups, degrees), F32),
        scratch_shapes=[
            pltpu.VMEM((groups, fields, group, halves, slots, degrees), F32),
            dma((groups,)),
        ],
        compiler_params=pltpu.CompilerParams(vmem_limit_bytes=16 * 1024 * 1024),
    )(landed, values, cols)


def solution(mesh):
    return jax.shard_map(
        body,
        mesh=mesh,
        in_specs=(
            P(None, "sub", None, "ma", None),
            P("ma"),
            P("sub", None, None, None, None),
            P("sub", None, None),
        ),
        out_specs=P(None, ("sub", "ma"), None, None, None),
        check_vma=False,
    )
```
